512 devices in a mesh: row: 16 (over z, y_lo), col: 32 (over y_hi, x, core).
Axes of the slice: x: 4, y: 8 (y_hi: 4, y_lo: 2; y = y_hi * 2 + y_lo), z: 8, core: 2. Of those that a mesh axis runs over, the one named last changes fastest.
Arguments:
- pressure: float32 [512, 1024, 512], P('row', 'col'), may hold values from -6 to 6
- cut_exponent: int32 [16, 32, 2], P('row', 'col'), may hold values from 0 to 3
- group_map: int32 [16, 32, 2], P('row', 'col'), may hold values from 0 to 15
Outputs:
- coeffs: float32 [512, 1024, 512], P('row', 'col')
- group_mass: float32 [16, 4], replicated
The draws below stay inside these ranges and needn't reach their ends.
Inputs may be any that keep to these rules, and one draw needn't show every extreme that they name: `cut_exponent`: one exponent per block of 32 x 32 x 512 // 2 cells.
All inputs are finite; a program needn't handle non-finite values.
Results may differ from the reference program's by a relative error of at most 0.0001.
Values sent between devices are 32-bit elements; how exact they have to be, the bound alone decides.
No kernel may reach another device: no remote copies, remote signals or barrier semaphores. Data moves between devices by JAX's collectives and lax.ppermute only.
A program may use at most 64 MiB of HBM per device.

```python
import jax
import jax.numpy as jnp
from jax import lax

CX = 32
CY = 32
CZ = 512
ZB = 2
GROUPS = 16
NX = 512
NY = 1024
N_ROW = 16
N_COL = 32


def with_ends(entries, rng, low, largest):
    dims = entries.shape
    place = [jax.random.randint(jax.random.fold_in(rng, axis), (), 0, dims[axis]) for axis in range(len(dims))]
    entries = entries.at[tuple(place)].set(low)
    longest = dims.index(max(dims))
    place[longest] = (place[longest] + 1) % dims[longest]
    return entries.at[tuple(place)].set(largest)


def block_scale(rng, shape, cuts, low, largest):
    def one(axis_at, blocks):
        steps = jax.random.uniform(jax.random.fold_in(jax.random.fold_in(rng, 6), axis_at), (blocks,), jnp.float32, low / len(cuts), largest / len(cuts))
        return jnp.repeat(jnp.exp(steps), shape[axis_at] // blocks).reshape((-1,) + (1,) * (len(shape) - axis_at - 1))

    gain = one(*cuts[0])
    for cut in cuts[1:]:
        gain = gain * one(*cut)
    return gain


def bell_draw(stream_key, shape, spread, most, cuts=(), held_as=jnp.bfloat16):
    values = jax.random.normal(stream_key, shape, jnp.float32) * spread
    if len(cuts) > 0:
        values = block_scale(stream_key, shape, cuts, -0.22, 0.18) * values
    return jnp.clip(values, min=-most, max=most).astype(held_as)


def setup_inputs(seed: int = 0) -> dict:
    splits = jax.random.split(jax.random.key(seed), 4)
    pressure = bell_draw(splits[0], (NX, NY, CZ), 1.0, 6.0, ((0, 16), (1, 32)), jnp.float32)
    cut_exponent = with_ends(jax.random.randint(splits[1], (N_ROW, N_COL, ZB), 0, 4), jax.random.fold_in(splits[1], 1), 0, 3).astype(jnp.int32)
    group_map = with_ends(jax.random.randint(splits[2], (N_ROW, N_COL, ZB), 0, GROUPS), jax.random.fold_in(splits[2], 1), 0, GROUPS - 1).astype(jnp.int32)
    return dict(pressure=pressure, cut_exponent=cut_exponent, group_map=group_map)


cut_levels = (0.25, 0.5, 1.0, 2.0)


def lift_axis(signal, axis_pos):
    length = signal.shape[axis_pos]
    evens_half = lax.slice_in_dim(signal, 0, length, stride=2, axis=axis_pos)
    odds_half = lax.slice_in_dim(signal, 1, length, stride=2, axis=axis_pos)
    guess = 0.5625 * (evens_half + jnp.roll(evens_half, -1, axis_pos)) - 0.0625 * (jnp.roll(evens_half, 1, axis_pos) + jnp.roll(evens_half, -2, axis_pos))
    detail = odds_half - guess
    smooth = evens_half + (0.28125 * (jnp.roll(detail, 1, axis_pos) + detail) - 0.03125 * (jnp.roll(detail, 2, axis_pos) + jnp.roll(detail, -1, axis_pos)))
    return jnp.stack([smooth, detail], axis_pos + 1).reshape(signal.shape)


def reference(pressure, cut_exponent, group_map):
    coeffs = lift_axis(pressure, 0)
    coeffs = lift_axis(coeffs, 1)
    coeffs = lift_axis(coeffs, 2)
    parity_x = (jnp.arange(NX, dtype=jnp.int32) % 2)[:, None, None]
    parity_y = (jnp.arange(NY, dtype=jnp.int32) % 2)[None, :, None]
    parity_z = (jnp.arange(CZ, dtype=jnp.int32) % 2)[None, None, :]
    detail_mask = (parity_x + parity_y + parity_z) > 0
    magnitude = jnp.where(detail_mask, jnp.abs(coeffs), jnp.float32(0.0))
    shaped = magnitude.reshape(N_ROW, CX, N_COL, CY, ZB, CZ // ZB)
    scales = jnp.exp2(-cut_exponent.astype(jnp.float32))
    cells = CX * CY * (CZ // ZB)
    block_list = []
    for level_value in cut_levels:
        limit = (level_value * scales)[:, None, :, None, :, None]
        block_list.append(jnp.sum(jnp.maximum(shaped - limit, 0.0), axis=(1, 3, 5)) / cells)
    block_mass = jnp.stack(block_list, -1)
    onehot = (group_map[..., None] == jnp.arange(GROUPS, dtype=jnp.int32)).astype(jnp.float32)
    group_mass = jnp.einsum("abzg,abzk->gk", onehot, block_mass.astype(jnp.float32), precision=lax.Precision.HIGHEST)
    return coeffs, group_mass
```

```python
import functools

import jax
import jax.numpy as jnp
from jax import lax
from jax.experimental import pallas as pl
from jax.experimental.pallas import tpu as pltpu
from jax.sharding import PartitionSpec as P

GROUPS = 16
LEVELS = (0.25, 0.5, 1.0, 2.0)
A, B, C, G = 0.5625, 0.0625, 0.28125, 0.03125
F32 = jnp.float32
VMEM = pl.BlockSpec(memory_space=pltpu.VMEM)
PARAMS = pltpu.CompilerParams(vmem_limit_bytes=16 << 20)
ANY = pl.BlockSpec(memory_space=pl.ANY)


def in_vmem(shape):
    return pltpu.VMEM(shape, F32)


def lane_lift(v):
    size = v.shape[-1]
    odd = lax.broadcasted_iota(jnp.int32, v.shape, 1) % 2 == 1
    near = pltpu.roll(v, 1, axis=1) + pltpu.roll(v, size - 1, axis=1)
    far = pltpu.roll(v, 3, axis=1) + pltpu.roll(v, size - 3, axis=1)
    w = jnp.where(odd, v - (A * near - B * far), v)
    near = pltpu.roll(w, 1, axis=1) + pltpu.roll(w, size - 1, axis=1)
    far = pltpu.roll(w, 3, axis=1) + pltpu.roll(w, size - 3, axis=1)
    return jnp.where(odd, w, w + (C * near - G * far))


def to_right(at):
    e0, o0, e1, o1, e2 = at(2), at(1), at(4), at(3), at(6)
    return e0, o0 - A * e0 + B * e1, o1 - A * (e1 + e0) + B * e2


def to_left(at):
    e0, o0, e1, e2 = at(0), at(1), at(2), at(4)
    return e0, e1, o0 - A * (e0 + e1) + B * e2


FROM_LEFT = {0: (C * B, C, -G), 1: (B, 0.0, 0.0), 2: (C * B, -G, 0.0), 4: (-G * B, 0.0, 0.0)}
FROM_RIGHT = {
    6: (-G * B, 0.0, 0.0),
    4: (C * B + G * A, -G * B, 0.0),
    3: (B, 0.0, 0.0),
    2: (C * (B - A), C * B, -G),
    1: (-A, B, 0.0),
}


def combine(coefs, lines):
    total = None
    for coef, line in zip(coefs, lines):
        if coef != 0.0:
            term = coef * line
            total = term if total is None else total + term
    return total


def edge_kernel(nx, ny, p_ref, right_ref, left_ref, first, last, sems):
    lo = pltpu.make_async_copy(p_ref.at[pl.ds(0, 5 * ny)], first, sems.at[0])
    hi = pltpu.make_async_copy(p_ref.at[pl.ds((nx - 6) * ny, 6 * ny)], last, sems.at[1])
    lo.start()
    hi.start()
    lo.wait()

    def left(t, _):
        rows = lambda x: pl.ds(pl.multiple_of(x * ny + t * 8, 8), 8)
        for k, v in enumerate(to_left(lambda i: first[rows(i), :])):
            left_ref[rows(k), :] = lane_lift(v)
        return 0

    lax.fori_loop(0, ny // 8, left, 0)
    hi.wait()

    def right(t, _):
        rows = lambda x: pl.ds(pl.multiple_of(x * ny + t * 8, 8), 8)
        for k, v in enumerate(to_right(lambda i: last[rows(6 - i), :])):
            right_ref[rows(k), :] = lane_lift(v)
        return 0

    lax.fori_loop(0, ny // 8, right, 0)


def row_partials(nx, ny, w_ref, x, slot, right_ref, left_ref):
    head = w_ref[pl.ds(pl.multiple_of(x * ny, 8), 8), :]
    tail = w_ref[pl.ds(pl.multiple_of(x * ny + ny - 8, 8), 8), :]
    for k, v in enumerate(to_right(lambda i: tail[8 - i : 9 - i, :])):
        right_ref[pl.ds(k * nx + slot, 1), :] = v
    for k, v in enumerate(to_left(lambda i: head[i : i + 1, :])):
        left_ref[pl.ds(k * nx + slot, 1), :] = v


def bulk_kernel(nx, ny, p_ref, after_ref, w_ref, right_ref, left_ref, raw, sems):
    del after_ref
    chunks = 4
    size = nx * ny // chunks
    copies = []
    for i in range(chunks):
        part = pl.ds(i * size, size)
        copies.append(pltpu.make_async_copy(p_ref.at[part], raw.at[part], sems.at[i]))
        copies[-1].start()
    for i in range(chunks):
        copies[i].wait()

        def depth(t, _):
            rows = pl.ds(pl.multiple_of(i * size + t * 8, 8), 8)
            w_ref[rows, :] = lane_lift(raw[rows, :])
            return 0

        lax.fori_loop(0, size // 8, depth, 0, unroll=2)
    half = nx // 2

    def column(t, _):
        for c in range(w_ref.shape[1] // 128):
            lanes = slice(c * 128, (c + 1) * 128)
            rows = lambda x: pl.ds(pl.multiple_of(x * ny + t * 8, 8), 8)
            e = [w_ref[rows(2 * j), lanes] for j in range(half)]
            d = {-2: B * e[0], -1: B * e[1] - A * e[0], half: B * e[half - 1]}
            for j in range(half):
                near = e[j] + e[j + 1] if j + 1 < half else e[j]
                v = w_ref[rows(2 * j + 1), lanes] - A * near
                far = [e[i] for i in (j - 1, j + 2) if 0 <= i < half]
                if far:
                    v = v + B * functools.reduce(lambda a, b: a + b, far)
                d[j] = v
                w_ref[rows(2 * j + 1), lanes] = v
            for j in range(half):
                w_ref[rows(2 * j), lanes] = e[j] + (C * (d[j - 1] + d[j]) - G * (d[j - 2] + d[j + 1]))
        return 0

    lax.fori_loop(0, ny // 8, column, 0)

    def partial(x, _):
        row_partials(nx, ny, w_ref, x, x, right_ref, left_ref)
        return 0

    lax.fori_loop(0, nx, partial, 0)


def plane_kernel(nx, ny, got_l_ref, got_r_ref, w_ref, right_in, left_in, fixed_ref, right_ref, left_ref):
    def fix(t, _):
        rows = lambda x: pl.ds(pl.multiple_of(x * ny + t * 8, 8), 8)
        lines = [got_l_ref[rows(k), :] for k in range(3)]
        for x in range(6):
            v = w_ref[rows(x), :]
            fixed_ref[rows(x), :] = v + combine(FROM_LEFT[x], lines) if x in FROM_LEFT else v
        lines = [got_r_ref[rows(k), :] for k in range(3)]
        for back in range(6, 0, -1):
            v = w_ref[rows(nx - back), :]
            fixed_ref[rows(12 - back), :] = v + combine(FROM_RIGHT[back], lines) if back in FROM_RIGHT else v
        return 0

    lax.fori_loop(0, ny // 8, fix, 0)
    right_ref[...] = right_in[...]
    left_ref[...] = left_in[...]
    for x in FROM_LEFT:
        row_partials(nx, ny, fixed_ref, x, x, right_ref, left_ref)
    for back in FROM_RIGHT:
        row_partials(nx, ny, fixed_ref, 12 - back, nx - back, right_ref, left_ref)


def excess(acc, v, even_plane, limits):
    m = jnp.abs(v)
    if even_plane:
        row = lax.broadcasted_iota(jnp.int32, v.shape, 0)
        lane = lax.broadcasted_iota(jnp.int32, v.shape, 1)
        m = jnp.where((row | lane) % 2 == 1, m, 0.0)
    return [a + jnp.maximum(m - lim, 0.0) for a, lim in zip(acc, limits)]


def rows_kernel(nx, ny, w_ref, fixed_ref, lim_ref, out_ref, edge_ref, acc_ref, mid, sems):
    size = w_ref.shape[1]
    acc_ref[...] = jnp.zeros_like(acc_ref)

    def lift(src, at_plane):
        v = src[pl.ds(pl.multiple_of(at_plane * ny, 8), ny), :]
        row = lax.broadcasted_iota(jnp.int32, v.shape, 0)
        odd = row % 2 == 1

        def at(u, by):
            r = pltpu.roll(u, -by % ny, axis=0)
            return jnp.where((row + by >= 0) & (row + by < ny), r, 0.0)

        near = at(v, -1) + at(v, 1)
        far = at(v, -3) + at(v, 3)
        w = jnp.where(odd, v - (A * near - B * far), v)
        near = at(w, -1) + at(w, 1)
        far = at(w, -3) + at(w, 3)
        s = w + (C * near - G * far)
        e0, e1, last = v[0:1, :], v[2:3, :], v[ny - 2 : ny - 1, :]
        before1, before2, after = B * e1 - A * e0, B * e0, B * last
        s = s + jnp.where(row == 0, C * before1 - G * before2, 0.0)
        s = s + jnp.where(row == 2, -G * before1, 0.0)
        s = s + jnp.where(row == ny - 2, -G * after, 0.0)
        return jnp.where(odd, w, s)

    def plane(src, at_plane, x, even_plane):
        v = lift(src, at_plane)
        edge_ref[pl.ds(pl.multiple_of(x * 16, 8), 8), :] = v[0:8, :]
        edge_ref[pl.ds(pl.multiple_of(x * 16 + 8, 8), 8), :] = v[ny - 8 : ny, :]
        mid[x] = v[8 : ny - 8, :]
        limits = [jnp.broadcast_to(lim_ref[l : l + 1, :], (8, size)) for l in range(4)]
        acc = [acc_ref[l] for l in range(4)]
        for t in range(1, ny // 8 - 1):
            acc = excess(acc, v[8 * t : 8 * t + 8, :], even_plane, limits)
        for l in range(4):
            acc_ref[l] = acc[l]

    copies = []
    middle = (nx - 12) // 2
    for i, (src, start, x0, each) in enumerate(
        ((fixed_ref, 0, 0, 6), (w_ref, 6, 6, middle), (w_ref, 6 + middle, 6 + middle, middle), (fixed_ref, 6, nx - 6, 6))
    ):

        def pair(j, _):
            plane(src, start + 2 * j, x0 + 2 * j, True)
            plane(src, start + 2 * j + 1, x0 + 2 * j + 1, False)
            return 0

        lax.fori_loop(0, each // 2, pair, 0)
        part = pl.ds(x0, each)
        copies.append(pltpu.make_async_copy(mid.at[part], out_ref.at[part, pl.ds(8, ny - 16), :], sems.at[i]))
        copies[-1].start()
    for copy in copies:
        copy.wait()


def final_kernel(nx, ny, scale, got_l_ref, got_r_ref, edge_ref, acc_in, lim_ref, hot_ref, out_in, out_ref, mass_ref, head, tail, acc_ref, sems):
    del out_in
    size = edge_ref.shape[1]
    row = lax.broadcasted_iota(jnp.int32, (8, size), 0)

    def weights(table, place, k):
        total = jnp.zeros((8, size), F32)
        for line, coefs in table.items():
            if coefs[k] != 0.0:
                total = jnp.where(row == place(line), coefs[k], total)
        return total

    from_l = [weights(FROM_LEFT, lambda i: i, k) for k in range(3)]
    from_r = [weights(FROM_RIGHT, lambda i: 8 - i, k) for k in range(3)]
    acc_ref[...] = acc_in[...]

    def tiles(x, even_plane):
        limits = [jnp.broadcast_to(lim_ref[l : l + 1, :], (8, size)) for l in range(4)]
        acc = [acc_ref[l] for l in range(4)]
        for got, table, dest, at in ((got_l_ref, from_l, head, 0), (got_r_ref, from_r, tail, 8)):
            v = edge_ref[pl.ds(pl.multiple_of(x * 16 + at, 8), 8), :]
            for k in range(3):
                v = v + table[k] * got[pl.ds(k * nx + x, 1), :]
            dest[x] = v
            acc = excess(acc, v, even_plane, limits)
        for l in range(4):
            acc_ref[l] = acc[l]

    parts = 4
    each = nx // parts
    copies = []
    for i in range(parts):

        def pair(j, _):
            tiles(i * each + 2 * j, True)
            tiles(i * each + 2 * j + 1, False)
            return 0

        lax.fori_loop(0, each // 2, pair, 0)
        part = pl.ds(i * each, each)
        for n, (src, at) in enumerate(((head, 0), (tail, ny - 8))):
            copies.append(pltpu.make_async_copy(src.at[part], out_ref.at[part, pl.ds(at, 8), :], sems.at[2 * i + n]))
            copies[-1].start()
    blocks = 2
    width = size // blocks
    lines = []
    for c in range(blocks):
        for l in range(4):
            lines.append(jnp.sum(acc_ref[l, :, c * width : (c + 1) * width], axis=0, keepdims=True))
    sums = jnp.sum(jnp.concatenate(lines, axis=0), axis=1, keepdims=True)
    line = jnp.sum(sums * hot_ref[...], axis=0, keepdims=True) * scale
    for i in range(mass_ref.shape[0]):
        mass_ref[i] = line
    for copy in copies:
        copy.wait()


def neighbours(value_up, value_down, axis):
    n = lax.axis_size(axis)
    up = [(i, (i + 1) % n) for i in range(n)]
    return lax.ppermute(value_up, axis, up), lax.ppermute(value_down, axis, [(j, i) for i, j in up])


def near(*values):
    return [pltpu.with_memory_space_constraint(v, pltpu.VMEM) for v in values]


def far(value):
    return pltpu.with_memory_space_constraint(value, pltpu.HBM)


def cost(flops):
    return pl.CostEstimate(flops=flops, bytes_accessed=4 << 20, transcendentals=0)


def shards(pressure, cut_exponent, group_map):
    nx, ny, size = pressure.shape
    flat = pressure.reshape(nx * ny, size)
    blocks_z = cut_exponent.shape[2]
    scales = jnp.exp2(-cut_exponent[0, 0].astype(F32))
    limits = jnp.repeat(jnp.array(LEVELS, F32)[:, None] * scales[None, :], size // blocks_z, axis=1)
    lane = jnp.arange(128, dtype=jnp.int32)[None, None, :]
    want = 4 * group_map[0, 0][:, None, None] + jnp.arange(4, dtype=jnp.int32)[None, :, None]
    hot = (lane == want).astype(F32).reshape(4 * blocks_z, 128)
    edge = pl.pallas_call(
        functools.partial(edge_kernel, nx, ny),
        out_shape=(in_vmem((3 * ny, size)), in_vmem((3 * ny, size))),
        in_specs=[ANY],
        out_specs=(VMEM, VMEM),
        scratch_shapes=[pltpu.VMEM((5 * ny, size), F32), pltpu.VMEM((6 * ny, size), F32), pltpu.SemaphoreType.DMA((2,))],
        compiler_params=PARAMS,
        name="edge",
    )
    right, left = edge(far(flat))
    from_left, from_right = neighbours(right, left, "row")
    bulk = pl.pallas_call(
        functools.partial(bulk_kernel, nx, ny),
        out_shape=(in_vmem((nx * ny, size)), in_vmem((3 * nx, size)), in_vmem((3 * nx, size))),
        in_specs=[ANY, VMEM],
        out_specs=(VMEM, VMEM, VMEM),
        scratch_shapes=[pltpu.VMEM((nx * ny, size), F32), pltpu.SemaphoreType.DMA((4,))],
        cost_estimate=cost(40_000_000),
        compiler_params=PARAMS,
        name="bulk",
    )
    work, right, left = bulk(far(flat), *near(right))
    plane = pl.pallas_call(
        functools.partial(plane_kernel, nx, ny),
        out_shape=(in_vmem((12 * ny, size)), in_vmem((3 * nx, size)), in_vmem((3 * nx, size))),
        in_specs=[VMEM] * 5,
        out_specs=(VMEM, VMEM, VMEM),
        compiler_params=PARAMS,
        name="plane",
    )
    fixed, right, left = plane(*near(from_left, from_right, work, right, left))
    from_left, from_right = neighbours(right, left, "col")
    rows = pl.pallas_call(
        functools.partial(rows_kernel, nx, ny),
        out_shape=(jax.ShapeDtypeStruct((nx, ny, size), F32), in_vmem((nx * 16, size)), in_vmem((4, 8, size))),
        in_specs=[VMEM, VMEM, VMEM],
        out_specs=(ANY, VMEM, VMEM),
        scratch_shapes=[pltpu.VMEM((nx, ny - 16, size), F32), pltpu.SemaphoreType.DMA((4,))],
        cost_estimate=cost(40_000_000),
        compiler_params=PARAMS,
        name="rows",
    )
    coeffs, edges, acc = rows(*near(work, fixed, limits))
    n_row, n_col = lax.axis_size("row"), lax.axis_size("col")
    scale = 1.0 / (nx * ny * (size // blocks_z))
    final = pl.pallas_call(
        functools.partial(final_kernel, nx, ny, scale),
        out_shape=(jax.ShapeDtypeStruct((nx, ny, size), F32), in_vmem((n_row, 1, 128))),
        in_specs=[VMEM] * 6 + [ANY],
        out_specs=(ANY, VMEM),
        input_output_aliases={6: 0},
        scratch_shapes=[
            pltpu.VMEM((nx, 8, size), F32),
            pltpu.VMEM((nx, 8, size), F32),
            pltpu.VMEM((4, 8, size), F32),
            pltpu.SemaphoreType.DMA((8,)),
        ],
        compiler_params=PARAMS,
        name="final",
    )
    coeffs, mass = final(*near(from_left, from_right, edges, acc, limits, hot), coeffs)
    mass = lax.all_to_all(mass, "row", 0, 0).sum(0, keepdims=True)
    mass = lax.all_to_all(jnp.broadcast_to(mass, (n_col, 1, 128)), "col", 0, 0).sum(0)
    return coeffs, mass[0, : 4 * GROUPS].reshape(GROUPS, 4)


def solution(mesh):
    split = P("row", "col", None)
    return jax.shard_map(shards, mesh=mesh, in_specs=(split, split, split), out_specs=(split, P()), check_vma=False)
```

```python
import functools

import jax
import jax.numpy as jnp
import numpy as np
from jax import lax
from jax.experimental import pallas as pl
from jax.experimental.pallas import tpu as pltpu
from jax.sharding import PartitionSpec as P

GROUPS = 16
LEVELS = (0.25, 0.5, 1.0, 2.0)
A, B, C, G = 0.5625, 0.0625, 0.28125, 0.03125
F32 = jnp.float32
VMEM = pl.BlockSpec(memory_space=pltpu.VMEM)
PARAMS = pltpu.CompilerParams(vmem_limit_bytes=16 << 20)
ANY = pl.BlockSpec(memory_space=pl.ANY)


def in_vmem(shape):
    return pltpu.VMEM(shape, F32)


def lane_lift(v):
    size = v.shape[-1]
    odd = lax.broadcasted_iota(jnp.int32, v.shape, 1) % 2 == 1
    near = pltpu.roll(v, 1, axis=1) + pltpu.roll(v, size - 1, axis=1)
    far = pltpu.roll(v, 3, axis=1) + pltpu.roll(v, size - 3, axis=1)
    w = jnp.where(odd, v - (A * near - B * far), v)
    near = pltpu.roll(w, 1, axis=1) + pltpu.roll(w, size - 1, axis=1)
    far = pltpu.roll(w, 3, axis=1) + pltpu.roll(w, size - 3, axis=1)
    return jnp.where(odd, w, w + (C * near - G * far))


def lane_table(size):
    shift = lambda m, by: np.roll(m, by, axis=1)
    ident = np.eye(size)
    e, o = ident[:, 0::2], ident[:, 1::2]
    d = o - A * (e + shift(e, -1)) + B * (shift(e, 1) + shift(e, -2))
    s = e + C * (shift(d, 1) + d) - G * (shift(d, 2) + shift(d, -1))
    return np.stack([s, d], axis=2).reshape(size, size).astype(jnp.bfloat16)


def table_lift(v, table):
    total = None
    for _ in range(3):
        piece = v.astype(jnp.bfloat16)
        v = v - piece.astype(F32)
        term = jnp.dot(piece, table, preferred_element_type=F32)
        total = term if total is None else total + term
    return total


def to_right(at):
    e0, o0, e1, o1, e2 = at(2), at(1), at(4), at(3), at(6)
    return e0, o0 - A * e0 + B * e1, o1 - A * (e1 + e0) + B * e2


def to_left(at):
    e0, o0, e1, e2 = at(0), at(1), at(2), at(4)
    return e0, e1, o0 - A * (e0 + e1) + B * e2


FROM_LEFT = {0: (C * B, C, -G), 1: (B, 0.0, 0.0), 2: (C * B, -G, 0.0), 4: (-G * B, 0.0, 0.0)}
FROM_RIGHT = {
    6: (-G * B, 0.0, 0.0),
    4: (C * B + G * A, -G * B, 0.0),
    3: (B, 0.0, 0.0),
    2: (C * (B - A), C * B, -G),
    1: (-A, B, 0.0),
}


def combine(coefs, lines):
    total = None
    for coef, line in zip(coefs, lines):
        if coef != 0.0:
            term = coef * line
            total = term if total is None else total + term
    return total


def edge_kernel(nx, ny, p_ref, right_ref, left_ref, first, last, sems):
    lo = pltpu.make_async_copy(p_ref.at[pl.ds(0, 5 * ny)], first, sems.at[0])
    hi = pltpu.make_async_copy(p_ref.at[pl.ds((nx - 6) * ny, 6 * ny)], last, sems.at[1])
    lo.start()
    hi.start()
    lo.wait()
    for k, v in enumerate(to_left(lambda i: first[pl.ds(i * ny, ny), :])):
        left_ref[pl.ds(k * ny, ny), :] = lane_lift(v)
    hi.wait()
    for k, v in enumerate(to_right(lambda i: last[pl.ds((6 - i) * ny, ny), :])):
        right_ref[pl.ds(k * ny, ny), :] = lane_lift(v)


def row_partials(nx, ny, w_ref, x, slot, right_ref, left_ref):
    head = w_ref[pl.ds(pl.multiple_of(x * ny, 8), 8), :]
    tail = w_ref[pl.ds(pl.multiple_of(x * ny + ny - 8, 8), 8), :]
    for k, v in enumerate(to_right(lambda i: tail[8 - i : 9 - i, :])):
        right_ref[pl.ds(k * nx + slot, 1), :] = v
    for k, v in enumerate(to_left(lambda i: head[i : i + 1, :])):
        left_ref[pl.ds(k * nx + slot, 1), :] = v


def bulk_kernel(nx, ny, p_ref, after_ref, table_ref, w_ref, right_ref, left_ref, raw, sems):
    del after_ref
    chunks = 4
    size = nx * ny // chunks
    copies = []
    for i in range(chunks):
        part = pl.ds(i * size, size)
        copies.append(pltpu.make_async_copy(p_ref.at[part], raw.at[part], sems.at[i]))
        copies[-1].start()
    for i in range(chunks):
        copies[i].wait()

        part = pl.ds(i * size, size)
        w_ref[part, :] = table_lift(raw[part, :], table_ref[...])
    half = nx // 2

    def column(t, _):
        for c in range(w_ref.shape[1] // 128):
            lanes = slice(c * 128, (c + 1) * 128)
            rows = lambda x: pl.ds(pl.multiple_of(x * ny + t * 8, 8), 8)
            e = [w_ref[rows(2 * j), lanes] for j in range(half)]
            d = {-2: B * e[0], -1: B * e[1] - A * e[0], half: B * e[half - 1]}
            for j in range(half):
                near = e[j] + e[j + 1] if j + 1 < half else e[j]
                v = w_ref[rows(2 * j + 1), lanes] - A * near
                far = [e[i] for i in (j - 1, j + 2) if 0 <= i < half]
                if far:
                    v = v + B * functools.reduce(lambda a, b: a + b, far)
                d[j] = v
                w_ref[rows(2 * j + 1), lanes] = v
            for j in range(half):
                w_ref[rows(2 * j), lanes] = e[j] + (C * (d[j - 1] + d[j]) - G * (d[j - 2] + d[j + 1]))
        return 0

    lax.fori_loop(0, ny // 8, column, 0)

    def partial(x, _):
        row_partials(nx, ny, w_ref, x, x, right_ref, left_ref)
        return 0

    lax.fori_loop(0, nx, partial, 0, unroll=4)


def plane_kernel(nx, ny, got_l_ref, got_r_ref, w_ref, right_in, left_in, fixed_ref, right_ref, left_ref):
    def fix(t, _):
        rows = lambda x: pl.ds(pl.multiple_of(x * ny + t * 8, 8), 8)
        lines = [got_l_ref[rows(k), :] for k in range(3)]
        for x in range(6):
            v = w_ref[rows(x), :]
            fixed_ref[rows(x), :] = v + combine(FROM_LEFT[x], lines) if x in FROM_LEFT else v
        lines = [got_r_ref[rows(k), :] for k in range(3)]
        for back in range(6, 0, -1):
            v = w_ref[rows(nx - back), :]
            fixed_ref[rows(12 - back), :] = v + combine(FROM_RIGHT[back], lines) if back in FROM_RIGHT else v
        return 0

    lax.fori_loop(0, ny // 8, fix, 0)
    right_ref[...] = right_in[...]
    left_ref[...] = left_in[...]
    for x in FROM_LEFT:
        row_partials(nx, ny, fixed_ref, x, x, right_ref, left_ref)
    for back in FROM_RIGHT:
        row_partials(nx, ny, fixed_ref, 12 - back, nx - back, right_ref, left_ref)


def excess(acc, v, even_plane, limits):
    m = jnp.abs(v)
    if even_plane:
        row = lax.broadcasted_iota(jnp.int32, v.shape, 0)
        lane = lax.broadcasted_iota(jnp.int32, v.shape, 1)
        m = jnp.where((row | lane) % 2 == 1, m, 0.0)
    return [a + jnp.maximum(m - lim, 0.0) for a, lim in zip(acc, limits)]


def rows_kernel(nx, ny, w_ref, fixed_ref, lim_ref, out_ref, edge_ref, acc_ref, mid, sems):
    size = w_ref.shape[1]
    acc_ref[...] = jnp.zeros_like(acc_ref)

    def lift(src, at_plane):
        v = src[pl.ds(pl.multiple_of(at_plane * ny, 8), ny), :]
        v = jnp.concatenate([v, jnp.zeros((8, size), F32)], axis=0)
        odd = lax.broadcasted_iota(jnp.int32, v.shape, 0) % 2 == 1
        at = lambda u, by: pltpu.roll(u, by % (ny + 8), axis=0)
        w = jnp.where(odd, v - (A * (at(v, 1) + at(v, -1)) - B * (at(v, 3) + at(v, -3))), v)
        s = w + (C * (at(w, 1) + at(w, -1)) - G * (at(w, 3) + at(w, -3)))
        return jnp.where(odd, w, s)[0:ny, :]

    def plane(src, at_plane, x, even_plane):
        v = lift(src, at_plane)
        edge_ref[pl.ds(pl.multiple_of(x * 16, 8), 8), :] = v[0:8, :]
        edge_ref[pl.ds(pl.multiple_of(x * 16 + 8, 8), 8), :] = v[ny - 8 : ny, :]
        mid[x] = v[8 : ny - 8, :]
        limits = [jnp.broadcast_to(lim_ref[l : l + 1, :], (8, size)) for l in range(4)]
        acc = [acc_ref[l] for l in range(4)]
        for t in range(1, ny // 8 - 1):
            acc = excess(acc, v[8 * t : 8 * t + 8, :], even_plane, limits)
        for l in range(4):
            acc_ref[l] = acc[l]

    copies = []
    middle = (nx - 12) // 2
    for i, (src, start, x0, each) in enumerate(
        ((fixed_ref, 0, 0, 6), (w_ref, 6, 6, middle), (w_ref, 6 + middle, 6 + middle, middle), (fixed_ref, 6, nx - 6, 6))
    ):

        def pair(j, _):
            plane(src, start + 2 * j, x0 + 2 * j, True)
            plane(src, start + 2 * j + 1, x0 + 2 * j + 1, False)
            return 0

        lax.fori_loop(0, each // 2, pair, 0)
        part = pl.ds(x0, each)
        copies.append(pltpu.make_async_copy(mid.at[part], out_ref.at[part, pl.ds(8, ny - 16), :], sems.at[i]))
        copies[-1].start()
    for copy in copies:
        copy.wait()


def final_kernel(nx, ny, scale, got_l_ref, got_r_ref, edge_ref, acc_in, lim_ref, hot_ref, out_in, out_ref, mass_ref, head, tail, acc_ref, sems):
    del out_in
    size = edge_ref.shape[1]
    row = lax.broadcasted_iota(jnp.int32, (8, size), 0)

    def weights(table, place, k):
        total = jnp.zeros((8, size), F32)
        for line, coefs in table.items():
            if coefs[k] != 0.0:
                total = jnp.where(row == place(line), coefs[k], total)
        return total

    from_l = [weights(FROM_LEFT, lambda i: i, k) for k in range(3)]
    from_r = [weights(FROM_RIGHT, lambda i: 8 - i, k) for k in range(3)]
    acc_ref[...] = acc_in[...]

    def tiles(x, even_plane):
        limits = [jnp.broadcast_to(lim_ref[l : l + 1, :], (8, size)) for l in range(4)]
        acc = [acc_ref[l] for l in range(4)]
        for got, table, dest, at in ((got_l_ref, from_l, head, 0), (got_r_ref, from_r, tail, 8)):
            v = edge_ref[pl.ds(pl.multiple_of(x * 16 + at, 8), 8), :]
            for k in range(3):
                v = v + table[k] * got[pl.ds(k * nx + x, 1), :]
            dest[x] = v
            acc = excess(acc, v, even_plane, limits)
        for l in range(4):
            acc_ref[l] = acc[l]

    parts = 4
    each = nx // parts
    copies = []
    for i in range(parts):

        def pair(j, _):
            tiles(i * each + 2 * j, True)
            tiles(i * each + 2 * j + 1, False)
            return 0

        lax.fori_loop(0, each // 2, pair, 0)
        part = pl.ds(i * each, each)
        for n, (src, at) in enumerate(((head, 0), (tail, ny - 8))):
            copies.append(pltpu.make_async_copy(src.at[part], out_ref.at[part, pl.ds(at, 8), :], sems.at[2 * i + n]))
            copies[-1].start()
    blocks = 2
    width = size // blocks
    lines = []
    for c in range(blocks):
        for l in range(4):
            lines.append(jnp.sum(acc_ref[l, :, c * width : (c + 1) * width], axis=0, keepdims=True))
    sums = jnp.sum(jnp.concatenate(lines, axis=0), axis=1, keepdims=True)
    sums = (sums * scale) * hot_ref[...]
    both = sums[0:4, :] + sums[4:8, :]
    for i in range(mass_ref.shape[0]):
        mass_ref[i] = both
    for copy in copies:
        copy.wait()


def neighbours(value_up, value_down, axis):
    n = lax.axis_size(axis)
    up = [(i, (i + 1) % n) for i in range(n)]
    return lax.ppermute(value_up, axis, up), lax.ppermute(value_down, axis, [(j, i) for i, j in up])


def near(*values):
    return [pltpu.with_memory_space_constraint(v, pltpu.VMEM) for v in values]


def far(value):
    return pltpu.with_memory_space_constraint(value, pltpu.HBM)


def cost(flops):
    return pl.CostEstimate(flops=flops, bytes_accessed=4 << 20, transcendentals=0)


def shards(pressure, cut_exponent, group_map):
    nx, ny, size = pressure.shape
    flat = pressure.reshape(nx * ny, size)
    blocks_z = cut_exponent.shape[2]
    scales = jnp.exp2(-cut_exponent[0, 0].astype(F32))
    limits = jnp.repeat(jnp.array(LEVELS, F32)[:, None] * scales[None, :], size // blocks_z, axis=1)
    hot = (jnp.arange(128, dtype=jnp.int32)[None, :] == jnp.repeat(group_map[0, 0], 4)[:, None]).astype(F32)
    edge = pl.pallas_call(
        functools.partial(edge_kernel, nx, ny),
        out_shape=(in_vmem((3 * ny, size)), in_vmem((3 * ny, size))),
        in_specs=[ANY],
        out_specs=(VMEM, VMEM),
        scratch_shapes=[pltpu.VMEM((5 * ny, size), F32), pltpu.VMEM((6 * ny, size), F32), pltpu.SemaphoreType.DMA((2,))],
        compiler_params=PARAMS,
        name="edge",
    )
    right, left = edge(far(flat))
    from_left, from_right = neighbours(right, left, "row")
    bulk = pl.pallas_call(
        functools.partial(bulk_kernel, nx, ny),
        out_shape=(in_vmem((nx * ny, size)), in_vmem((3 * nx, size)), in_vmem((3 * nx, size))),
        in_specs=[ANY, VMEM, VMEM],
        out_specs=(VMEM, VMEM, VMEM),
        scratch_shapes=[pltpu.VMEM((nx * ny, size), F32), pltpu.SemaphoreType.DMA((4,))],
        cost_estimate=cost(40_000_000),
        compiler_params=PARAMS,
        name="bulk",
    )
    work, right, left = bulk(far(flat), *near(right, jnp.asarray(lane_table(size))))
    plane = pl.pallas_call(
        functools.partial(plane_kernel, nx, ny),
        out_shape=(in_vmem((12 * ny, size)), in_vmem((3 * nx, size)), in_vmem((3 * nx, size))),
        in_specs=[VMEM] * 5,
        out_specs=(VMEM, VMEM, VMEM),
        compiler_params=PARAMS,
        name="plane",
    )
    fixed, right, left = plane(*near(from_left, from_right, work, right, left))
    from_left, from_right = neighbours(right, left, "col")
    rows = pl.pallas_call(
        functools.partial(rows_kernel, nx, ny),
        out_shape=(jax.ShapeDtypeStruct((nx, ny, size), F32), in_vmem((nx * 16, size)), in_vmem((4, 8, size))),
        in_specs=[VMEM, VMEM, VMEM],
        out_specs=(ANY, VMEM, VMEM),
        scratch_shapes=[pltpu.VMEM((nx, ny - 16, size), F32), pltpu.SemaphoreType.DMA((4,))],
        cost_estimate=cost(40_000_000),
        compiler_params=PARAMS,
        name="rows",
    )
    coeffs, edges, acc = rows(*near(work, fixed, limits))
    n_row, n_col = lax.axis_size("row"), lax.axis_size("col")
    scale = 1.0 / (nx * ny * (size // blocks_z))
    final = pl.pallas_call(
        functools.partial(final_kernel, nx, ny, scale),
        out_shape=(jax.ShapeDtypeStruct((nx, ny, size), F32), in_vmem((n_row, 4, 128))),
        in_specs=[VMEM] * 6 + [ANY],
        out_specs=(ANY, VMEM),
        input_output_aliases={6: 0},
        scratch_shapes=[
            pltpu.VMEM((nx, 8, size), F32),
            pltpu.VMEM((nx, 8, size), F32),
            pltpu.VMEM((4, 8, size), F32),
            pltpu.SemaphoreType.DMA((8,)),
        ],
        compiler_params=PARAMS,
        name="final",
    )
    coeffs, mass = final(*near(from_left, from_right, edges, acc, limits, hot), coeffs)
    mass = lax.all_to_all(mass, "row", 0, 0).sum(0)
    mass = lax.all_to_all(jnp.broadcast_to(mass, (n_col, 4, 128)), "col", 0, 0).sum(0)
    return coeffs, mass[:, :GROUPS].T


def solution(mesh):
    split = P("row", "col", None)
    return jax.shard_map(shards, mesh=mesh, in_specs=(split, split, split), out_specs=(split, P()), check_vma=False)
```

```python
import functools

import jax
import jax.numpy as jnp
import numpy as np
from jax import lax
from jax.experimental import pallas as pl
from jax.experimental.pallas import tpu as pltpu
from jax.sharding import Mesh
from jax.sharding import PartitionSpec as P

GROUPS = 16
ROW = ("z", "y_lo")
COL = ("y_hi", "x", "core")
FIRST = ("y_hi", "y_lo", "core")
SECOND = ("z", "x")
LEVELS = (0.25, 0.5, 1.0, 2.0)
A, B, C, G = 0.5625, 0.0625, 0.28125, 0.03125
F32 = jnp.float32
VMEM = pl.BlockSpec(memory_space=pltpu.VMEM)
PARAMS = pltpu.CompilerParams(vmem_limit_bytes=16 << 20)
ANY = pl.BlockSpec(memory_space=pl.ANY)


def in_vmem(shape):
    return pltpu.VMEM(shape, F32)


def lane_lift(v):
    size = v.shape[-1]
    odd = lax.broadcasted_iota(jnp.int32, v.shape, 1) % 2 == 1
    near = pltpu.roll(v, 1, axis=1) + pltpu.roll(v, size - 1, axis=1)
    far = pltpu.roll(v, 3, axis=1) + pltpu.roll(v, size - 3, axis=1)
    w = jnp.where(odd, v - (A * near - B * far), v)
    near = pltpu.roll(w, 1, axis=1) + pltpu.roll(w, size - 1, axis=1)
    far = pltpu.roll(w, 3, axis=1) + pltpu.roll(w, size - 3, axis=1)
    return jnp.where(odd, w, w + (C * near - G * far))


def lane_table(size):
    shift = lambda m, by: np.roll(m, by, axis=1)
    ident = np.eye(size)
    e, o = ident[:, 0::2], ident[:, 1::2]
    d = o - A * (e + shift(e, -1)) + B * (shift(e, 1) + shift(e, -2))
    s = e + C * (shift(d, 1) + d) - G * (shift(d, 2) + shift(d, -1))
    return np.stack([s, d], axis=2).reshape(size, size).astype(jnp.bfloat16)


def table_lift(v, table):
    total = None
    for _ in range(3):
        piece = v.astype(jnp.bfloat16)
        v = v - piece.astype(F32)
        term = jnp.dot(piece, table, preferred_element_type=F32)
        total = term if total is None else total + term
    return total


def to_right(at):
    e0, o0, e1, o1, e2 = at(2), at(1), at(4), at(3), at(6)
    return e0, o0 - A * e0 + B * e1, o1 - A * (e1 + e0) + B * e2


def to_left(at):
    e0, o0, e1, e2 = at(0), at(1), at(2), at(4)
    return e0, e1, o0 - A * (e0 + e1) + B * e2


FROM_LEFT = {0: (C * B, C, -G), 1: (B, 0.0, 0.0), 2: (C * B, -G, 0.0), 4: (-G * B, 0.0, 0.0)}
FROM_RIGHT = {
    6: (-G * B, 0.0, 0.0),
    4: (C * B + G * A, -G * B, 0.0),
    3: (B, 0.0, 0.0),
    2: (C * (B - A), C * B, -G),
    1: (-A, B, 0.0),
}


def combine(coefs, lines):
    total = None
    for coef, line in zip(coefs, lines):
        if coef != 0.0:
            term = coef * line
            total = term if total is None else total + term
    return total


def edge_kernel(nx, ny, p_ref, right_ref, left_ref, first, last, sems):
    lo = pltpu.make_async_copy(p_ref.at[pl.ds(0, 5 * ny)], first, sems.at[0])
    hi = pltpu.make_async_copy(p_ref.at[pl.ds((nx - 6) * ny, 6 * ny)], last, sems.at[1])
    lo.start()
    hi.start()
    lo.wait()
    for k, v in enumerate(to_left(lambda i: first[pl.ds(i * ny, ny), :])):
        left_ref[pl.ds(k * ny, ny), :] = lane_lift(v)
    hi.wait()
    for k, v in enumerate(to_right(lambda i: last[pl.ds((6 - i) * ny, ny), :])):
        right_ref[pl.ds(k * ny, ny), :] = lane_lift(v)


def row_partials(nx, ny, w_ref, x, slot, inner_ref, outer_ref):
    even = lax.axis_index("core") == 0
    head = w_ref[pl.ds(pl.multiple_of(x * ny, 8), 8), :]
    tail = w_ref[pl.ds(pl.multiple_of(x * ny + ny - 8, 8), 8), :]
    right = to_right(lambda i: tail[8 - i : 9 - i, :])
    left = to_left(lambda i: head[i : i + 1, :])
    for k, (r, l) in enumerate(zip(right, left)):
        inner_ref[pl.ds(k * nx + slot, 1), :] = jnp.where(even, r, l)
        outer_ref[pl.ds(k * nx + slot, 1), :] = jnp.where(even, l, r)


def bulk_kernel(nx, ny, p_ref, after_ref, table_ref, w_ref, inner_ref, outer_ref, raw, sems):
    del after_ref
    chunks = 4
    size = nx * ny // chunks
    copies = []
    for i in range(chunks):
        part = pl.ds(i * size, size)
        copies.append(pltpu.make_async_copy(p_ref.at[part], raw.at[part], sems.at[i]))
        copies[-1].start()
    for i in range(chunks):
        copies[i].wait()

        part = pl.ds(i * size, size)
        w_ref[part, :] = table_lift(raw[part, :], table_ref[...])
    half = nx // 2

    def column(t, _):
        for c in range(w_ref.shape[1] // 128):
            lanes = slice(c * 128, (c + 1) * 128)
            rows = lambda x: pl.ds(pl.multiple_of(x * ny + t * 8, 8), 8)
            e = [w_ref[rows(2 * j), lanes] for j in range(half)]
            d = {-2: B * e[0], -1: B * e[1] - A * e[0], half: B * e[half - 1]}
            for j in range(half):
                near = e[j] + e[j + 1] if j + 1 < half else e[j]
                v = w_ref[rows(2 * j + 1), lanes] - A * near
                far = [e[i] for i in (j - 1, j + 2) if 0 <= i < half]
                if far:
                    v = v + B * functools.reduce(lambda a, b: a + b, far)
                d[j] = v
                w_ref[rows(2 * j + 1), lanes] = v
            for j in range(half):
                w_ref[rows(2 * j), lanes] = e[j] + (C * (d[j - 1] + d[j]) - G * (d[j - 2] + d[j + 1]))
        return 0

    lax.fori_loop(0, ny // 8, column, 0)

    def partial(x, _):
        row_partials(nx, ny, w_ref, x, x, inner_ref, outer_ref)
        return 0

    lax.fori_loop(0, nx, partial, 0, unroll=4)


def plane_kernel(nx, ny, got_l_ref, got_r_ref, w_ref, inner_in, outer_in, fixed_ref, inner_ref, outer_ref):
    def fix(t, _):
        rows = lambda x: pl.ds(pl.multiple_of(x * ny + t * 8, 8), 8)
        lines = [got_l_ref[rows(k), :] for k in range(3)]
        for x in range(6):
            v = w_ref[rows(x), :]
            fixed_ref[rows(x), :] = v + combine(FROM_LEFT[x], lines) if x in FROM_LEFT else v
        lines = [got_r_ref[rows(k), :] for k in range(3)]
        for back in range(6, 0, -1):
            v = w_ref[rows(nx - back), :]
            fixed_ref[rows(12 - back), :] = v + combine(FROM_RIGHT[back], lines) if back in FROM_RIGHT else v
        return 0

    lax.fori_loop(0, ny // 8, fix, 0)
    inner_ref[...] = inner_in[...]
    outer_ref[...] = outer_in[...]
    for x in FROM_LEFT:
        row_partials(nx, ny, fixed_ref, x, x, inner_ref, outer_ref)
    for back in FROM_RIGHT:
        row_partials(nx, ny, fixed_ref, 12 - back, nx - back, inner_ref, outer_ref)


def excess(acc, v, even_plane, limits):
    m = jnp.abs(v)
    if even_plane:
        row = lax.broadcasted_iota(jnp.int32, v.shape, 0)
        lane = lax.broadcasted_iota(jnp.int32, v.shape, 1)
        m = jnp.where((row | lane) % 2 == 1, m, 0.0)
    return [a + jnp.maximum(m - lim, 0.0) for a, lim in zip(acc, limits)]


def rows_kernel(nx, ny, w_ref, fixed_ref, lim_ref, out_ref, edge_ref, acc_ref, mid, sems):
    size = w_ref.shape[1]
    acc_ref[...] = jnp.zeros_like(acc_ref)

    def lift(src, at_plane):
        v = src[pl.ds(pl.multiple_of(at_plane * ny, 8), ny), :]
        v = jnp.concatenate([v, jnp.zeros((8, size), F32)], axis=0)
        odd = lax.broadcasted_iota(jnp.int32, v.shape, 0) % 2 == 1
        at = lambda u, by: pltpu.roll(u, by % (ny + 8), axis=0)
        w = jnp.where(odd, v - (A * (at(v, 1) + at(v, -1)) - B * (at(v, 3) + at(v, -3))), v)
        s = w + (C * (at(w, 1) + at(w, -1)) - G * (at(w, 3) + at(w, -3)))
        return jnp.where(odd, w, s)[0:ny, :]

    def plane(src, at_plane, x, even_plane):
        v = lift(src, at_plane)
        edge_ref[pl.ds(pl.multiple_of(x * 16, 8), 8), :] = v[0:8, :]
        edge_ref[pl.ds(pl.multiple_of(x * 16 + 8, 8), 8), :] = v[ny - 8 : ny, :]
        mid[x] = v[8 : ny - 8, :]
        limits = [jnp.broadcast_to(lim_ref[l : l + 1, :], (8, size)) for l in range(4)]
        acc = [acc_ref[l] for l in range(4)]
        for t in range(1, ny // 8 - 1):
            acc = excess(acc, v[8 * t : 8 * t + 8, :], even_plane, limits)
        for l in range(4):
            acc_ref[l] = acc[l]

    copies = []
    middle = (nx - 12) // 2
    for i, (src, start, x0, each) in enumerate(
        ((fixed_ref, 0, 0, 6), (w_ref, 6, 6, middle), (w_ref, 6 + middle, 6 + middle, middle), (fixed_ref, 6, nx - 6, 6))
    ):

        def pair(j, _):
            plane(src, start + 2 * j, x0 + 2 * j, True)
            plane(src, start + 2 * j + 1, x0 + 2 * j + 1, False)
            return 0

        lax.fori_loop(0, each // 2, pair, 0)
        part = pl.ds(x0, each)
        copies.append(pltpu.make_async_copy(mid.at[part], out_ref.at[part, pl.ds(8, ny - 16), :], sems.at[i]))
        copies[-1].start()
    for copy in copies:
        copy.wait()


def final_kernel(nx, ny, scale, outer_ref, inner_ref, edge_ref, acc_in, lim_ref, hot_ref, out_in, out_ref, mass_ref, head, tail, acc_ref, sems):
    del out_in
    size = edge_ref.shape[1]
    row = lax.broadcasted_iota(jnp.int32, (8, size), 0)

    def weights(table, place, k):
        total = jnp.zeros((8, size), F32)
        for line, coefs in table.items():
            if coefs[k] != 0.0:
                total = jnp.where(row == place(line), coefs[k], total)
        return total

    from_l = [weights(FROM_LEFT, lambda i: i, k) for k in range(3)]
    from_r = [weights(FROM_RIGHT, lambda i: 8 - i, k) for k in range(3)]
    acc_ref[...] = acc_in[...]
    even = lax.axis_index("core") == 0

    def tiles(x, even_plane):
        limits = [jnp.broadcast_to(lim_ref[l : l + 1, :], (8, size)) for l in range(4)]
        acc = [acc_ref[l] for l in range(4)]
        inner = [inner_ref[pl.ds(k * nx + x, 1), :] for k in range(3)]
        outer = [outer_ref[pl.ds(k * nx + x, 1), :] for k in range(3)]
        left = [jnp.where(even, o, i) for i, o in zip(inner, outer)]
        right = [jnp.where(even, i, o) for i, o in zip(inner, outer)]
        for got, table, dest, at in ((left, from_l, head, 0), (right, from_r, tail, 8)):
            v = edge_ref[pl.ds(pl.multiple_of(x * 16 + at, 8), 8), :]
            for k in range(3):
                v = v + table[k] * got[k]
            dest[x] = v
            acc = excess(acc, v, even_plane, limits)
        for l in range(4):
            acc_ref[l] = acc[l]

    parts = 4
    each = nx // parts
    copies = []
    for i in range(parts):

        def pair(j, _):
            tiles(i * each + 2 * j, True)
            tiles(i * each + 2 * j + 1, False)
            return 0

        lax.fori_loop(0, each // 2, pair, 0)
        part = pl.ds(i * each, each)
        for n, (src, at) in enumerate(((head, 0), (tail, ny - 8))):
            copies.append(pltpu.make_async_copy(src.at[part], out_ref.at[part, pl.ds(at, 8), :], sems.at[2 * i + n]))
            copies[-1].start()
    blocks = 2
    width = size // blocks
    lines = []
    for c in range(blocks):
        for l in range(4):
            lines.append(jnp.sum(acc_ref[l, :, c * width : (c + 1) * width], axis=0, keepdims=True))
    sums = jnp.sum(jnp.concatenate(lines, axis=0), axis=1, keepdims=True)
    line = jnp.sum((sums * scale) * hot_ref[...], axis=0, keepdims=True)
    for i in range(mass_ref.shape[0]):
        mass_ref[i] = line
    for copy in copies:
        copy.wait()


def neighbours(value_up, value_down, axis):
    n = lax.axis_size(axis)
    up = [(i, (i + 1) % n) for i in range(n)]
    return lax.ppermute(value_up, axis, up), lax.ppermute(value_down, axis, [(j, i) for i, j in up])


def pair_swaps(n):
    inner = [(i, i ^ 1) for i in range(n)]
    return inner, [((i + 1) % n, (j + 1) % n) for i, j in inner]


def near(*values):
    return [pltpu.with_memory_space_constraint(v, pltpu.VMEM) for v in values]


def far(value):
    return pltpu.with_memory_space_constraint(value, pltpu.HBM)


def cost(flops):
    return pl.CostEstimate(flops=flops, bytes_accessed=4 << 20, transcendentals=0)


def shards(pressure, cut_exponent, group_map):
    nx, ny, size = pressure.shape
    flat = pressure.reshape(nx * ny, size)
    blocks_z = cut_exponent.shape[2]
    scales = jnp.exp2(-cut_exponent[0, 0].astype(F32))
    limits = jnp.repeat(jnp.array(LEVELS, F32)[:, None] * scales[None, :], size // blocks_z, axis=1)
    level = jnp.tile(jnp.arange(4, dtype=jnp.int32), blocks_z)
    place = GROUPS * level + jnp.repeat(group_map[0, 0], 4)
    hot = (jnp.arange(128, dtype=jnp.int32)[None, :] == place[:, None]).astype(F32)
    edge = pl.pallas_call(
        functools.partial(edge_kernel, nx, ny),
        out_shape=(in_vmem((3 * ny, size)), in_vmem((3 * ny, size))),
        in_specs=[ANY],
        out_specs=(VMEM, VMEM),
        scratch_shapes=[pltpu.VMEM((5 * ny, size), F32), pltpu.VMEM((6 * ny, size), F32), pltpu.SemaphoreType.DMA((2,))],
        compiler_params=PARAMS,
        name="edge",
    )
    right, left = edge(far(flat))
    from_left, from_right = neighbours(right, left, ROW)
    bulk = pl.pallas_call(
        functools.partial(bulk_kernel, nx, ny),
        out_shape=(in_vmem((nx * ny, size)), in_vmem((3 * nx, size)), in_vmem((3 * nx, size))),
        in_specs=[ANY, VMEM, VMEM],
        out_specs=(VMEM, VMEM, VMEM),
        scratch_shapes=[pltpu.VMEM((nx * ny, size), F32), pltpu.SemaphoreType.DMA((4,))],
        cost_estimate=cost(40_000_000),
        compiler_params=PARAMS,
        name="bulk",
    )
    work, inner, outer = bulk(far(flat), *near(right, jnp.asarray(lane_table(size))))
    plane = pl.pallas_call(
        functools.partial(plane_kernel, nx, ny),
        out_shape=(in_vmem((12 * ny, size)), in_vmem((3 * nx, size)), in_vmem((3 * nx, size))),
        in_specs=[VMEM] * 5,
        out_specs=(VMEM, VMEM, VMEM),
        compiler_params=PARAMS,
        name="plane",
    )
    fixed, inner, outer = plane(*near(from_left, from_right, work, inner, outer))
    swap_inner, swap_outer = pair_swaps(lax.axis_size(COL))
    inner = lax.ppermute(inner, COL, swap_inner)
    outer = lax.ppermute(outer, COL, swap_outer)
    rows = pl.pallas_call(
        functools.partial(rows_kernel, nx, ny),
        out_shape=(jax.ShapeDtypeStruct((nx, ny, size), F32), in_vmem((nx * 16, size)), in_vmem((4, 8, size))),
        in_specs=[VMEM, VMEM, VMEM],
        out_specs=(ANY, VMEM, VMEM),
        scratch_shapes=[pltpu.VMEM((nx, ny - 16, size), F32), pltpu.SemaphoreType.DMA((4,))],
        cost_estimate=cost(40_000_000),
        compiler_params=PARAMS,
        name="rows",
    )
    coeffs, edges, acc = rows(*near(work, fixed, limits))
    n_first, n_second = lax.axis_size(FIRST), lax.axis_size(SECOND)
    scale = 1.0 / (nx * ny * (size // blocks_z))
    final = pl.pallas_call(
        functools.partial(final_kernel, nx, ny, scale),
        out_shape=(jax.ShapeDtypeStruct((nx, ny, size), F32), in_vmem((n_first, 1, 128))),
        in_specs=[VMEM] * 6 + [ANY],
        out_specs=(ANY, VMEM),
        input_output_aliases={6: 0},
        scratch_shapes=[
            pltpu.VMEM((nx, 8, size), F32),
            pltpu.VMEM((nx, 8, size), F32),
            pltpu.VMEM((4, 8, size), F32),
            pltpu.SemaphoreType.DMA((8,)),
        ],
        compiler_params=PARAMS,
        name="final",
    )
    coeffs, mass = final(*near(outer, inner, edges, acc, limits, hot), coeffs)
    mass = lax.all_to_all(mass, FIRST, 0, 0).sum(0)
    mass = lax.all_to_all(jnp.broadcast_to(mass, (n_second, 1, 128)), SECOND, 0, 0).sum(0)
    return coeffs, mass[0, : 4 * GROUPS].reshape(4, GROUPS).T


def solution(mesh):
    rows, cols = mesh.devices.shape
    z, y_hi = rows // 2, max(cols // 8, 1)
    devices = mesh.devices.reshape(z, 2, y_hi, cols // 2 // y_hi, 2)
    split = P(ROW, COL, None)
    return jax.shard_map(
        shards,
        mesh=Mesh(devices, ROW + COL),
        in_specs=(split, split, split),
        out_specs=(split, P()),
        check_vma=False,
    )
```

```python
import functools

import jax
import jax.numpy as jnp
import numpy as np
from jax import lax
from jax.experimental import pallas as pl
from jax.experimental.pallas import tpu as pltpu
from jax.sharding import Mesh
from jax.sharding import PartitionSpec as P

GROUPS = 16
ROW = ("z", "y_lo")
COL = ("y_hi", "x", "core")
FIRST = ("y_hi", "y_lo", "core")
SECOND = ("z", "x")
LEVELS = (0.25, 0.5, 1.0, 2.0)
A, B, C, G = 0.5625, 0.0625, 0.28125, 0.03125
F32 = jnp.float32
VMEM = pl.BlockSpec(memory_space=pltpu.VMEM)
PARAMS = pltpu.CompilerParams(vmem_limit_bytes=16 << 20)
ANY = pl.BlockSpec(memory_space=pl.ANY)


def in_vmem(shape):
    return pltpu.VMEM(shape, F32)


def lane_lift(v):
    size = v.shape[-1]
    odd = lax.broadcasted_iota(jnp.int32, v.shape, 1) % 2 == 1
    near = pltpu.roll(v, 1, axis=1) + pltpu.roll(v, size - 1, axis=1)
    far = pltpu.roll(v, 3, axis=1) + pltpu.roll(v, size - 3, axis=1)
    w = jnp.where(odd, v - (A * near - B * far), v)
    near = pltpu.roll(w, 1, axis=1) + pltpu.roll(w, size - 1, axis=1)
    far = pltpu.roll(w, 3, axis=1) + pltpu.roll(w, size - 3, axis=1)
    return jnp.where(odd, w, w + (C * near - G * far))


def lane_table(size):
    shift = lambda m, by: np.roll(m, by, axis=1)
    ident = np.eye(size)
    e, o = ident[:, 0::2], ident[:, 1::2]
    d = o - A * (e + shift(e, -1)) + B * (shift(e, 1) + shift(e, -2))
    s = e + C * (shift(d, 1) + d) - G * (shift(d, 2) + shift(d, -1))
    return np.stack([s, d], axis=2).reshape(size, size).astype(jnp.bfloat16)


def table_lift(v, table):
    total = None
    for _ in range(3):
        piece = v.astype(jnp.bfloat16)
        v = v - piece.astype(F32)
        term = jnp.dot(piece, table, preferred_element_type=F32)
        total = term if total is None else total + term
    return total


def to_right(at):
    e0, o0, e1, o1, e2 = at(2), at(1), at(4), at(3), at(6)
    return e0, o0 - A * e0 + B * e1, o1 - A * (e1 + e0) + B * e2


def to_left(at):
    e0, o0, e1, e2 = at(0), at(1), at(2), at(4)
    return e0, e1, o0 - A * (e0 + e1) + B * e2


FROM_LEFT = {0: (C * B, C, -G), 1: (B, 0.0, 0.0), 2: (C * B, -G, 0.0), 4: (-G * B, 0.0, 0.0)}
FROM_RIGHT = {
    6: (-G * B, 0.0, 0.0),
    4: (C * B + G * A, -G * B, 0.0),
    3: (B, 0.0, 0.0),
    2: (C * (B - A), C * B, -G),
    1: (-A, B, 0.0),
}


def combine(coefs, lines):
    total = None
    for coef, line in zip(coefs, lines):
        if coef != 0.0:
            term = coef * line
            total = term if total is None else total + term
    return total


def edge_kernel(nx, ny, p_ref, right_ref, left_ref, first, last, sems):
    lo = pltpu.make_async_copy(p_ref.at[pl.ds(0, 5 * ny)], first, sems.at[0])
    hi = pltpu.make_async_copy(p_ref.at[pl.ds((nx - 6) * ny, 6 * ny)], last, sems.at[1])
    lo.start()
    hi.start()
    lo.wait()
    for k, v in enumerate(to_left(lambda i: first[pl.ds(i * ny, ny), :])):
        left_ref[pl.ds(k * ny, ny), :] = v
    hi.wait()
    for k, v in enumerate(to_right(lambda i: last[pl.ds((6 - i) * ny, ny), :])):
        right_ref[pl.ds(k * ny, ny), :] = v


def boundary_lines(head, tail):
    return (*to_right(lambda i: tail[8 - i : 9 - i, :]), *to_left(lambda i: head[i : i + 1, :]))


def edge_weights(size):
    row = lax.broadcasted_iota(jnp.int32, (8, size), 0)

    def weights(table, place, k):
        total = jnp.zeros((8, size), F32)
        for line, coefs in table.items():
            if coefs[k] != 0.0:
                total = jnp.where(row == place(line), coefs[k], total)
        return total

    head = [weights(FROM_LEFT, lambda i: i, k) for k in range(3)]
    return head, [weights(FROM_RIGHT, lambda i: 8 - i, k) for k in range(3)]


def bulk_kernel(nx, ny, p_ref, after_ref, table_ref, w_ref, inner_ref, outer_ref, raw, sems):
    del after_ref
    chunks = 4
    size = nx * ny // chunks
    copies = []
    for i in range(chunks):
        part = pl.ds(i * size, size)
        copies.append(pltpu.make_async_copy(p_ref.at[part], raw.at[part], sems.at[i]))
        copies[-1].start()
    for i in range(chunks):
        copies[i].wait()

        part = pl.ds(i * size, size)
        w_ref[part, :] = table_lift(raw[part, :], table_ref[...])
    half = nx // 2

    def column(t, _):
        for c in range(w_ref.shape[1] // 128):
            lanes = slice(c * 128, (c + 1) * 128)
            rows = lambda x: pl.ds(pl.multiple_of(x * ny + t * 8, 8), 8)
            e = [w_ref[rows(2 * j), lanes] for j in range(half)]
            d = {-2: B * e[0], -1: B * e[1] - A * e[0], half: B * e[half - 1]}
            for j in range(half):
                near = e[j] + e[j + 1] if j + 1 < half else e[j]
                v = w_ref[rows(2 * j + 1), lanes] - A * near
                far = [e[i] for i in (j - 1, j + 2) if 0 <= i < half]
                if far:
                    v = v + B * functools.reduce(lambda a, b: a + b, far)
                d[j] = v
                w_ref[rows(2 * j + 1), lanes] = v
            for j in range(half):
                w_ref[rows(2 * j), lanes] = e[j] + (C * (d[j - 1] + d[j]) - G * (d[j - 2] + d[j + 1]))
        return 0

    lax.fori_loop(0, ny // 8, column, 0)

    even = lax.axis_index("core") == 0

    def partial(x, _):
        head = w_ref[pl.ds(pl.multiple_of(x * ny, 8), 8), :]
        tail = w_ref[pl.ds(pl.multiple_of(x * ny + ny - 8, 8), 8), :]
        lines = boundary_lines(head, tail)
        for k, (right, left) in enumerate(zip(lines[:3], lines[3:])):
            inner_ref[pl.ds(k * nx + x, 1), :] = jnp.where(even, right, left)
            outer_ref[pl.ds(k * nx + x, 1), :] = jnp.where(even, left, right)
        return 0

    lax.fori_loop(0, nx, partial, 0, unroll=4)


def plane_kernel(nx, ny, got_l_ref, got_r_ref, table_ref, inner_in, outer_in, inner_ref, outer_ref, lines):
    size = table_ref.shape[0]
    even = lax.axis_index("core") == 0
    lines[...] = jnp.zeros_like(lines)
    for h in range(6):
        got = (got_l_ref, got_r_ref)[h // 3]
        at = h % 3 * ny
        for m, line in enumerate(boundary_lines(got[at : at + 8, :], got[at + ny - 8 : at + ny, :])):
            lines[6 * h + m : 6 * h + m + 1, :] = line
    lines[...] = table_lift(lines[...], table_ref[...])
    inner_ref[...] = inner_in[...]
    outer_ref[...] = outer_in[...]
    for first, at, weights in zip((0, 3), (0, nx - 8), edge_weights(size)):
        for k in range(3):
            row = lambda h, m: lines[6 * h + m : 6 * h + m + 1, :]
            right = sum(weights[i] * row(first + i, k) for i in range(3))
            left = sum(weights[i] * row(first + i, 3 + k) for i in range(3))
            part = slice(k * nx + at, k * nx + at + 8)
            inner_ref[part, :] = inner_ref[part, :] + jnp.where(even, right, left)
            outer_ref[part, :] = outer_ref[part, :] + jnp.where(even, left, right)


def excess(acc, v, even_plane, limits):
    m = jnp.abs(v)
    if even_plane:
        row = lax.broadcasted_iota(jnp.int32, v.shape, 0)
        lane = lax.broadcasted_iota(jnp.int32, v.shape, 1)
        m = jnp.where((row | lane) % 2 == 1, m, 0.0)
    return [a + jnp.maximum(m - lim, 0.0) for a, lim in zip(acc, limits)]


def rows_kernel(nx, ny, w_ref, got_l_ref, got_r_ref, table_ref, cut_ref, group_ref, out_ref, acc_ref, lim_ref, hot_ref, halo, fixed_ref):
    size = w_ref.shape[1]
    blocks = cut_ref.shape[1]
    lane = lax.broadcasted_iota(jnp.int32, (1, size), 1)
    cut = jnp.zeros((1, size), jnp.int32)
    place = lax.broadcasted_iota(jnp.int32, (8, 128), 0)
    group = jnp.zeros((8, 128), jnp.int32)
    for c in range(blocks):
        cut = jnp.where(lane // (size // blocks) == c, cut_ref[:, c : c + 1], cut)
        group = jnp.where(place // 4 == c, group_ref[:, c : c + 1], group)
    scales = jnp.exp2(-cut.astype(F32))
    for l, level in enumerate(LEVELS):
        lim_ref[l : l + 1, :] = level * scales
    hot = lax.broadcasted_iota(jnp.int32, (8, 128), 1) == GROUPS * (place % 4) + group
    hot_ref[...] = jnp.where(hot, 1.0, 0.0)
    acc_ref[...] = jnp.zeros_like(acc_ref)

    halo[pl.ds(0, 3 * ny), :] = table_lift(got_l_ref[...], table_ref[...])
    halo[pl.ds(3 * ny, 3 * ny), :] = table_lift(got_r_ref[...], table_ref[...])

    def fix(t, _):
        rows = lambda x: pl.ds(pl.multiple_of(x * ny + t * 8, 8), 8)
        lines = [halo[rows(k), :] for k in range(3)]
        for x in range(6):
            v = w_ref[rows(x), :]
            fixed_ref[rows(x), :] = v + combine(FROM_LEFT[x], lines) if x in FROM_LEFT else v
        lines = [halo[rows(3 + k), :] for k in range(3)]
        for back in range(6, 0, -1):
            v = w_ref[rows(nx - back), :]
            fixed_ref[rows(12 - back), :] = v + combine(FROM_RIGHT[back], lines) if back in FROM_RIGHT else v
        return 0

    lax.fori_loop(0, ny // 8, fix, 0)

    def lift(src, at_plane):
        v = src[pl.ds(pl.multiple_of(at_plane * ny, 8), ny), :]
        v = jnp.concatenate([v, jnp.zeros((8, size), F32)], axis=0)
        odd = lax.broadcasted_iota(jnp.int32, v.shape, 0) % 2 == 1
        at = lambda u, by: pltpu.roll(u, by % (ny + 8), axis=0)
        w = jnp.where(odd, v - (A * (at(v, 1) + at(v, -1)) - B * (at(v, 3) + at(v, -3))), v)
        s = w + (C * (at(w, 1) + at(w, -1)) - G * (at(w, 3) + at(w, -3)))
        return jnp.where(odd, w, s)[0:ny, :]

    def plane(src, at_plane, x, even_plane):
        v = lift(src, at_plane)
        out_ref[pl.ds(pl.multiple_of(x * ny, 8), ny), :] = v
        limits = [jnp.broadcast_to(lim_ref[l : l + 1, :], (8, size)) for l in range(4)]
        acc = [acc_ref[l] for l in range(4)]
        for t in range(1, ny // 8 - 1):
            acc = excess(acc, v[8 * t : 8 * t + 8, :], even_plane, limits)
        for l in range(4):
            acc_ref[l] = acc[l]

    for src, start, x0, each in ((fixed_ref, 0, 0, 6), (w_ref, 6, 6, nx - 12), (fixed_ref, 6, nx - 6, 6)):

        def pair(j, _):
            plane(src, start + 2 * j, x0 + 2 * j, True)
            plane(src, start + 2 * j + 1, x0 + 2 * j + 1, False)
            return 0

        lax.fori_loop(0, each // 2, pair, 0)


def final_kernel(nx, ny, scale, outer_ref, inner_ref, acc_in, lim_ref, hot_ref, base_ref, out_ref, mass_ref, acc_ref):
    size = base_ref.shape[1]
    from_l, from_r = edge_weights(size)
    acc_ref[...] = acc_in[...]
    even = lax.axis_index("core") == 0

    def tiles(x, even_plane):
        limits = [jnp.broadcast_to(lim_ref[l : l + 1, :], (8, size)) for l in range(4)]
        acc = [acc_ref[l] for l in range(4)]
        inner = [inner_ref[pl.ds(k * nx + x, 1), :] for k in range(3)]
        outer = [outer_ref[pl.ds(k * nx + x, 1), :] for k in range(3)]
        left = [jnp.where(even, o, i) for i, o in zip(inner, outer)]
        right = [jnp.where(even, i, o) for i, o in zip(inner, outer)]
        for got, table, at in ((left, from_l, 0), (right, from_r, ny - 8)):
            part = pl.ds(pl.multiple_of(x * ny + at, 8), 8)
            v = base_ref[part, :]
            for k in range(3):
                v = v + table[k] * got[k]
            out_ref[part, :] = v
            acc = excess(acc, v, even_plane, limits)
        for l in range(4):
            acc_ref[l] = acc[l]

    def pair(j, _):
        tiles(2 * j, True)
        tiles(2 * j + 1, False)
        return 0

    lax.fori_loop(0, nx // 2, pair, 0, unroll=2)
    blocks = 2
    width = size // blocks
    lines = []
    for c in range(blocks):
        for l in range(4):
            lines.append(jnp.sum(acc_ref[l, :, c * width : (c + 1) * width], axis=0, keepdims=True))
    sums = jnp.sum(jnp.concatenate(lines, axis=0), axis=1, keepdims=True)
    line = jnp.sum((sums * scale) * hot_ref[...], axis=0, keepdims=True)
    for i in range(mass_ref.shape[0]):
        mass_ref[i] = line


def neighbours(value_up, value_down, axis):
    n = lax.axis_size(axis)
    up = [(i, (i + 1) % n) for i in range(n)]
    return lax.ppermute(value_up, axis, up), lax.ppermute(value_down, axis, [(j, i) for i, j in up])


def pair_swaps(n):
    inner = [(i, i ^ 1) for i in range(n)]
    return inner, [((i + 1) % n, (j + 1) % n) for i, j in inner]


def near(*values):
    return [pltpu.with_memory_space_constraint(v, pltpu.VMEM) for v in values]


def far(value):
    return pltpu.with_memory_space_constraint(value, pltpu.HBM)


def cost(flops):
    return pl.CostEstimate(flops=flops, bytes_accessed=4 << 20, transcendentals=0)


def shards(pressure, cut_exponent, group_map):
    nx, ny, size = pressure.shape
    flat = pressure.reshape(nx * ny, size)
    blocks_z = cut_exponent.shape[2]
    table = jnp.asarray(lane_table(size))
    edge = pl.pallas_call(
        functools.partial(edge_kernel, nx, ny),
        out_shape=(in_vmem((3 * ny, size)), in_vmem((3 * ny, size))),
        in_specs=[ANY],
        out_specs=(VMEM, VMEM),
        scratch_shapes=[pltpu.VMEM((5 * ny, size), F32), pltpu.VMEM((6 * ny, size), F32), pltpu.SemaphoreType.DMA((2,))],
        compiler_params=PARAMS,
        name="edge",
    )
    right, left = edge(far(flat))
    from_left, from_right = neighbours(right, left, ROW)
    bulk = pl.pallas_call(
        functools.partial(bulk_kernel, nx, ny),
        out_shape=(in_vmem((nx * ny, size)), in_vmem((3 * nx, size)), in_vmem((3 * nx, size))),
        in_specs=[ANY, VMEM, VMEM],
        out_specs=(VMEM, VMEM, VMEM),
        scratch_shapes=[pltpu.VMEM((nx * ny, size), F32), pltpu.SemaphoreType.DMA((4,))],
        cost_estimate=cost(40_000_000),
        compiler_params=PARAMS,
        name="bulk",
    )
    work, inner, outer = bulk(far(flat), *near(right, table))
    plane = pl.pallas_call(
        functools.partial(plane_kernel, nx, ny),
        out_shape=(in_vmem((3 * nx, size)), in_vmem((3 * nx, size))),
        in_specs=[VMEM] * 5,
        out_specs=(VMEM, VMEM),
        scratch_shapes=[pltpu.VMEM((40, size), F32)],
        compiler_params=PARAMS,
        name="plane",
    )
    inner, outer = plane(*near(from_left, from_right, table, inner, outer))
    swap_inner, swap_outer = pair_swaps(lax.axis_size(COL))
    inner = lax.ppermute(inner, COL, swap_inner)
    outer = lax.ppermute(outer, COL, swap_outer)
    rows = pl.pallas_call(
        functools.partial(rows_kernel, nx, ny),
        out_shape=(in_vmem((nx * ny, size)), in_vmem((4, 8, size)), in_vmem((4, size)), in_vmem((8, 128))),
        in_specs=[VMEM] * 6,
        out_specs=(VMEM,) * 4,
        scratch_shapes=[pltpu.VMEM((6 * ny, size), F32), pltpu.VMEM((12 * ny, size), F32)],
        cost_estimate=cost(40_000_000),
        compiler_params=PARAMS,
        name="rows",
    )
    base, acc, limits, hot = rows(
        *near(work, from_left, from_right, table, cut_exponent.reshape(1, blocks_z), group_map.reshape(1, blocks_z))
    )
    n_first, n_second = lax.axis_size(FIRST), lax.axis_size(SECOND)
    scale = 1.0 / (nx * ny * (size // blocks_z))
    final = pl.pallas_call(
        functools.partial(final_kernel, nx, ny, scale),
        out_shape=(in_vmem((nx * ny, size)), in_vmem((n_first, 1, 128))),
        in_specs=[VMEM] * 6,
        out_specs=(VMEM, VMEM),
        input_output_aliases={5: 0},
        scratch_shapes=[pltpu.VMEM((4, 8, size), F32)],
        compiler_params=PARAMS,
        name="final",
    )
    coeffs, mass = final(*near(outer, inner, acc, limits, hot, base))
    mass = lax.all_to_all(mass, FIRST, 0, 0).sum(0)
    mass = lax.all_to_all(jnp.broadcast_to(mass, (n_second, 1, 128)), SECOND, 0, 0).sum(0)
    return coeffs.reshape(nx, ny, size), mass[0, : 4 * GROUPS].reshape(4, GROUPS).T


def solution(mesh):
    rows, cols = mesh.devices.shape
    z, y_hi = rows // 2, max(cols // 8, 1)
    devices = mesh.devices.reshape(z, 2, y_hi, cols // 2 // y_hi, 2)
    split = P(ROW, COL, None)
    return jax.shard_map(
        shards,
        mesh=Mesh(devices, ROW + COL),
        in_specs=(split, split, split),
        out_specs=(split, P()),
        check_vma=False,
    )
```

```python
import functools

import jax
import jax.numpy as jnp
import numpy as np
from jax import lax
from jax.experimental import pallas as pl
from jax.experimental.pallas import tpu as pltpu
from jax.sharding import Mesh
from jax.sharding import PartitionSpec as P

GROUPS = 16
ROW = ("z", "y_lo")
COL = ("y_hi", "x", "core")
FIRST = ("y_hi", "y_lo", "core")
SECOND = ("z", "x")
LEVELS = (0.25, 0.5, 1.0, 2.0)
A, B, C, G = 0.5625, 0.0625, 0.28125, 0.03125
F32 = jnp.float32
VMEM = pl.BlockSpec(memory_space=pltpu.VMEM)
PARAMS = pltpu.CompilerParams(vmem_limit_bytes=16 << 20)
ANY = pl.BlockSpec(memory_space=pl.ANY)


def in_vmem(shape, dtype=F32):
    return pltpu.VMEM(shape, dtype)


def lane_lift(v):
    size = v.shape[-1]
    odd = lax.broadcasted_iota(jnp.int32, v.shape, 1) % 2 == 1
    near = pltpu.roll(v, 1, axis=1) + pltpu.roll(v, size - 1, axis=1)
    far = pltpu.roll(v, 3, axis=1) + pltpu.roll(v, size - 3, axis=1)
    w = jnp.where(odd, v - (A * near - B * far), v)
    near = pltpu.roll(w, 1, axis=1) + pltpu.roll(w, size - 1, axis=1)
    far = pltpu.roll(w, 3, axis=1) + pltpu.roll(w, size - 3, axis=1)
    return jnp.where(odd, w, w + (C * near - G * far))


def lane_table(size):
    shift = lambda m, by: np.roll(m, by, axis=1)
    ident = np.eye(size)
    e, o = ident[:, 0::2], ident[:, 1::2]
    d = o - A * (e + shift(e, -1)) + B * (shift(e, 1) + shift(e, -2))
    s = e + C * (shift(d, 1) + d) - G * (shift(d, 2) + shift(d, -1))
    return np.stack([s, d], axis=2).reshape(size, size).astype(jnp.bfloat16)


def table_lift(v, table, pieces=2):
    total = None
    for _ in range(pieces):
        piece = v.astype(jnp.bfloat16)
        v = v - piece.astype(F32)
        term = jnp.dot(piece, table, preferred_element_type=F32)
        total = term if total is None else total + term
    return total


def to_right(at):
    e0, o0, e1, o1, e2 = at(2), at(1), at(4), at(3), at(6)
    return e0, o0 - A * e0 + B * e1, o1 - A * (e1 + e0) + B * e2


def to_left(at):
    e0, o0, e1, e2 = at(0), at(1), at(2), at(4)
    return e0, e1, o0 - A * (e0 + e1) + B * e2


FROM_LEFT = {0: (C * B, C, -G), 1: (B, 0.0, 0.0), 2: (C * B, -G, 0.0), 4: (-G * B, 0.0, 0.0)}
FROM_RIGHT = {
    6: (-G * B, 0.0, 0.0),
    4: (C * B + G * A, -G * B, 0.0),
    3: (B, 0.0, 0.0),
    2: (C * (B - A), C * B, -G),
    1: (-A, B, 0.0),
}


def combine(coefs, lines):
    total = None
    for coef, line in zip(coefs, lines):
        if coef != 0.0:
            term = coef * line
            total = term if total is None else total + term
    return total


def edge_kernel(nx, ny, p_ref, outer_ref, inner_ref, first, last, sems):
    lo = pltpu.make_async_copy(p_ref.at[pl.ds(0, 5 * ny)], first, sems.at[0])
    hi = pltpu.make_async_copy(p_ref.at[pl.ds((nx - 6) * ny, 6 * ny)], last, sems.at[1])
    lo.start()
    hi.start()
    even = lax.axis_index("y_lo") == 0
    lo.wait()
    hi.wait()
    left = to_left(lambda i: first[pl.ds(i * ny, ny), :])
    right = to_right(lambda i: last[pl.ds((6 - i) * ny, ny), :])
    for k, (r, l) in enumerate(zip(right, left)):
        outer_ref[pl.ds(k * ny, ny), :] = jnp.where(even, l, r)
        inner_ref[pl.ds(k * ny, ny), :] = jnp.where(even, r, l)


def boundary_lines(head, tail):
    return (*to_right(lambda i: tail[8 - i : 9 - i, :]), *to_left(lambda i: head[i : i + 1, :]))


def edge_weights(size):
    row = lax.broadcasted_iota(jnp.int32, (8, size), 0)

    def weights(table, place, k):
        total = jnp.zeros((8, size), F32)
        for line, coefs in table.items():
            if coefs[k] != 0.0:
                total = jnp.where(row == place(line), coefs[k], total)
        return total

    head = [weights(FROM_LEFT, lambda i: i, k) for k in range(3)]
    return head, [weights(FROM_RIGHT, lambda i: 8 - i, k) for k in range(3)]


def bulk_kernel(nx, ny, p_ref, table_hbm, w_ref, inner_ref, outer_ref, table_ref, sem):
    copy = pltpu.make_async_copy(table_hbm, table_ref, sem)
    copy.start()
    half = nx // 2
    tiles = w_ref.shape[1] // 128

    def column(i, _):
        lanes = pl.ds(pl.multiple_of(i % tiles * 128, 128), 128)
        rows = lambda x: pl.ds(pl.multiple_of(x * ny + i // tiles * 8, 8), 8)
        e = [p_ref[rows(2 * j), lanes] for j in range(half)]
        d = {-2: B * e[0], -1: B * e[1] - A * e[0], half: B * e[half - 1]}
        for j in range(half):
            near = e[j] + e[j + 1] if j + 1 < half else e[j]
            v = p_ref[rows(2 * j + 1), lanes] - A * near
            far = [e[i] for i in (j - 1, j + 2) if 0 <= i < half]
            if far:
                v = v + B * functools.reduce(lambda a, b: a + b, far)
            d[j] = v
            w_ref[rows(2 * j + 1), lanes] = v
        for j in range(half):
            w_ref[rows(2 * j), lanes] = e[j] + (C * (d[j - 1] + d[j]) - G * (d[j - 2] + d[j + 1]))
        return 0

    lax.fori_loop(0, ny // 8 * tiles, column, 0, unroll=2)
    copy.wait()
    size = nx * ny // 4
    for i in range(4):
        part = pl.ds(i * size, size)
        w_ref[part, :] = table_lift(w_ref[part, :], table_ref[...], 3)
    even = lax.axis_index("core") == 0

    def partial(x, _):
        head = w_ref[pl.ds(pl.multiple_of(x * ny, 8), 8), :]
        tail = w_ref[pl.ds(pl.multiple_of(x * ny + ny - 8, 8), 8), :]
        lines = boundary_lines(head, tail)
        for k, (right, left) in enumerate(zip(lines[:3], lines[3:])):
            inner_ref[pl.ds(k * nx + x, 1), :] = jnp.where(even, right, left)
            outer_ref[pl.ds(k * nx + x, 1), :] = jnp.where(even, left, right)
        return 0

    lax.fori_loop(0, nx, partial, 0, unroll=8)


def plane_kernel(nx, ny, got_o_ref, got_i_ref, table_ref, inner_in, outer_in, inner_ref, outer_ref, lines):
    size = table_ref.shape[0]
    even = lax.axis_index("core") == 0
    lines[...] = jnp.zeros_like(lines)
    y_even = lax.axis_index("y_lo") == 0
    for h in range(6):
        at = h % 3 * ny
        of_even, of_odd = (got_o_ref, got_i_ref) if h < 3 else (got_i_ref, got_o_ref)
        got = lambda part: jnp.where(y_even, of_even[part, :], of_odd[part, :])
        for m, line in enumerate(boundary_lines(got(slice(at, at + 8)), got(slice(at + ny - 8, at + ny)))):
            lines[6 * h + m : 6 * h + m + 1, :] = line
    lines[...] = table_lift(lines[...], table_ref[...])
    inner_ref[...] = inner_in[...]
    outer_ref[...] = outer_in[...]
    for first, at, weights in zip((0, 3), (0, nx - 8), edge_weights(size)):
        for k in range(3):
            row = lambda h, m: lines[6 * h + m : 6 * h + m + 1, :]
            right = sum(weights[i] * row(first + i, k) for i in range(3))
            left = sum(weights[i] * row(first + i, 3 + k) for i in range(3))
            part = slice(k * nx + at, k * nx + at + 8)
            inner_ref[part, :] = inner_ref[part, :] + jnp.where(even, right, left)
            outer_ref[part, :] = outer_ref[part, :] + jnp.where(even, left, right)


def excess(acc, v, even_plane, limits):
    m = jnp.abs(v)
    if even_plane:
        row = lax.broadcasted_iota(jnp.int32, v.shape, 0)
        lane = lax.broadcasted_iota(jnp.int32, v.shape, 1)
        m = jnp.where((row | lane) % 2 == 1, m, 0.0)
    return [a + jnp.maximum(m - lim, 0.0) for a, lim in zip(acc, limits)]


def rows_kernel(nx, ny, w_ref, got_o_ref, got_i_ref, table_ref, cut_ref, group_ref, out_ref, acc_ref, lim_ref, hot_ref, halo, fixed_ref):
    size = w_ref.shape[1]
    blocks = cut_ref.shape[1]
    lane = lax.broadcasted_iota(jnp.int32, (1, size), 1)
    cut = jnp.zeros((1, size), jnp.int32)
    place = lax.broadcasted_iota(jnp.int32, (8, 128), 0)
    group = jnp.zeros((8, 128), jnp.int32)
    for c in range(blocks):
        cut = jnp.where(lane // (size // blocks) == c, cut_ref[:, c : c + 1], cut)
        group = jnp.where(place // 4 == c, group_ref[:, c : c + 1], group)
    scales = jnp.exp2(-cut.astype(F32))
    for l, level in enumerate(LEVELS):
        lim_ref[l : l + 1, :] = level * scales
    hot = lax.broadcasted_iota(jnp.int32, (8, 128), 1) == GROUPS * (place % 4) + group
    hot_ref[...] = jnp.where(hot, 1.0, 0.0)
    acc_ref[...] = jnp.zeros_like(acc_ref)

    y_even = lax.axis_index("y_lo") == 0
    halo[pl.ds(0, 3 * ny), :] = table_lift(jnp.where(y_even, got_o_ref[...], got_i_ref[...]), table_ref[...])
    halo[pl.ds(3 * ny, 3 * ny), :] = table_lift(jnp.where(y_even, got_i_ref[...], got_o_ref[...]), table_ref[...])

    def fix(t, _):
        rows = lambda x: pl.ds(pl.multiple_of(x * ny + t * 8, 8), 8)
        lines = [halo[rows(k), :] for k in range(3)]
        for x in range(6):
            v = w_ref[rows(x), :]
            fixed_ref[rows(x), :] = v + combine(FROM_LEFT[x], lines) if x in FROM_LEFT else v
        lines = [halo[rows(3 + k), :] for k in range(3)]
        for back in range(6, 0, -1):
            v = w_ref[rows(nx - back), :]
            fixed_ref[rows(12 - back), :] = v + combine(FROM_RIGHT[back], lines) if back in FROM_RIGHT else v
        return 0

    lax.fori_loop(0, ny // 8, fix, 0)

    def lift(src, at_plane):
        v = src[pl.ds(pl.multiple_of(at_plane * ny, 8), ny), :]
        v = jnp.concatenate([v, jnp.zeros((8, size), F32)], axis=0)
        odd = lax.broadcasted_iota(jnp.int32, v.shape, 0) % 2 == 1
        at = lambda u, by: pltpu.roll(u, by % (ny + 8), axis=0)
        w = jnp.where(odd, v - (A * (at(v, 1) + at(v, -1)) - B * (at(v, 3) + at(v, -3))), v)
        s = w + (C * (at(w, 1) + at(w, -1)) - G * (at(w, 3) + at(w, -3)))
        return jnp.where(odd, w, s)[0:ny, :]

    def plane(src, at_plane, x, even_plane):
        v = lift(src, at_plane)
        out_ref[pl.ds(pl.multiple_of(x * ny, 8), ny), :] = v
        limits = [jnp.broadcast_to(lim_ref[l : l + 1, :], (8, size)) for l in range(4)]
        acc = [acc_ref[l] for l in range(4)]
        for t in range(1, ny // 8 - 1):
            acc = excess(acc, v[8 * t : 8 * t + 8, :], even_plane, limits)
        for l in range(4):
            acc_ref[l] = acc[l]

    for src, start, x0, each in ((fixed_ref, 0, 0, 6), (w_ref, 6, 6, nx - 12), (fixed_ref, 6, nx - 6, 6)):

        def pair(j, _):
            plane(src, start + 2 * j, x0 + 2 * j, True)
            plane(src, start + 2 * j + 1, x0 + 2 * j + 1, False)
            return 0

        lax.fori_loop(0, each // 2, pair, 0)


def final_kernel(nx, ny, scale, outer_ref, inner_ref, acc_in, lim_ref, hot_ref, base_ref, out_ref, mass_ref, acc_ref):
    size = base_ref.shape[1]
    from_l, from_r = edge_weights(size)
    acc_ref[...] = acc_in[...]
    even = lax.axis_index("core") == 0

    def tiles(x, even_plane):
        limits = [jnp.broadcast_to(lim_ref[l : l + 1, :], (8, size)) for l in range(4)]
        acc = [acc_ref[l] for l in range(4)]
        inner = [inner_ref[pl.ds(k * nx + x, 1), :] for k in range(3)]
        outer = [outer_ref[pl.ds(k * nx + x, 1), :] for k in range(3)]
        left = [jnp.where(even, o, i) for i, o in zip(inner, outer)]
        right = [jnp.where(even, i, o) for i, o in zip(inner, outer)]
        for got, table, at in ((left, from_l, 0), (right, from_r, ny - 8)):
            part = pl.ds(pl.multiple_of(x * ny + at, 8), 8)
            v = base_ref[part, :]
            for k in range(3):
                v = v + table[k] * got[k]
            out_ref[part, :] = v
            acc = excess(acc, v, even_plane, limits)
        for l in range(4):
            acc_ref[l] = acc[l]

    def pair(j, _):
        tiles(2 * j, True)
        tiles(2 * j + 1, False)
        return 0

    lax.fori_loop(0, nx // 2, pair, 0, unroll=2)
    blocks = 2
    width = size // blocks
    lines = []
    for c in range(blocks):
        for l in range(4):
            lines.append(jnp.sum(acc_ref[l, :, c * width : (c + 1) * width], axis=0, keepdims=True))
    sums = jnp.sum(jnp.concatenate(lines, axis=0), axis=1, keepdims=True)
    line = jnp.sum((sums * scale) * hot_ref[...], axis=0, keepdims=True)
    for i in range(mass_ref.shape[0]):
        mass_ref[i] = line


def spread_kernel(parts_ref, out_ref):
    total = parts_ref[0]
    for i in range(1, parts_ref.shape[0]):
        total = total + parts_ref[i]
    for i in range(out_ref.shape[0]):
        out_ref[i] = total


def pair_swaps(n):
    inner = [(i, i ^ 1) for i in range(n)]
    return inner, [((i + 1) % n, (j + 1) % n) for i, j in inner]


def exchange(outer, inner, axes):
    swap_inner, swap_outer = pair_swaps(lax.axis_size(axes))
    inner = lax.ppermute(inner, axes, swap_inner)
    return lax.ppermute(outer, axes, swap_outer), inner


def near(*values):
    return [pltpu.with_memory_space_constraint(v, pltpu.VMEM) for v in values]


def far(value):
    return pltpu.with_memory_space_constraint(value, pltpu.HBM)


def cost(flops):
    return pl.CostEstimate(flops=flops, bytes_accessed=4 << 20, transcendentals=0)


def shards(pressure, cut_exponent, group_map):
    nx, ny, size = pressure.shape
    flat = pressure.reshape(nx * ny, size)
    blocks_z = cut_exponent.shape[2]
    table = jnp.asarray(lane_table(size))
    edge = pl.pallas_call(
        functools.partial(edge_kernel, nx, ny),
        out_shape=(in_vmem((3 * ny, size)), in_vmem((3 * ny, size))),
        in_specs=[ANY],
        out_specs=(VMEM, VMEM),
        scratch_shapes=[pltpu.VMEM((5 * ny, size), F32), pltpu.VMEM((6 * ny, size), F32), pltpu.SemaphoreType.DMA((2,))],
        compiler_params=PARAMS,
        name="edge",
    )
    outer, inner = edge(far(flat))
    later, outer, inner = lax.optimization_barrier((flat, outer, inner))
    got_outer, got_inner = exchange(outer, inner, ROW)
    bulk = pl.pallas_call(
        functools.partial(bulk_kernel, nx, ny),
        out_shape=(
            in_vmem((nx * ny, size)),
            in_vmem((3 * nx, size)),
            in_vmem((3 * nx, size)),
            in_vmem((size, size), jnp.bfloat16),
        ),
        in_specs=[VMEM, ANY],
        out_specs=(VMEM,) * 4,
        scratch_shapes=[pltpu.SemaphoreType.DMA],
        cost_estimate=cost(40_000_000),
        compiler_params=PARAMS,
        name="bulk",
    )
    work, inner, outer, table = bulk(*near(later), far(table))
    plane = pl.pallas_call(
        functools.partial(plane_kernel, nx, ny),
        out_shape=(in_vmem((3 * nx, size)), in_vmem((3 * nx, size))),
        in_specs=[VMEM] * 5,
        out_specs=(VMEM, VMEM),
        scratch_shapes=[pltpu.VMEM((40, size), F32)],
        compiler_params=PARAMS,
        name="plane",
    )
    inner, outer = plane(*near(got_outer, got_inner, table, inner, outer))
    outer, inner = exchange(outer, inner, COL)
    rows = pl.pallas_call(
        functools.partial(rows_kernel, nx, ny),
        out_shape=(in_vmem((nx * ny, size)), in_vmem((4, 8, size)), in_vmem((4, size)), in_vmem((8, 128))),
        in_specs=[VMEM] * 6,
        out_specs=(VMEM,) * 4,
        scratch_shapes=[pltpu.VMEM((6 * ny, size), F32), pltpu.VMEM((12 * ny, size), F32)],
        cost_estimate=cost(40_000_000),
        compiler_params=PARAMS,
        name="rows",
    )
    base, acc, limits, hot = rows(
        *near(work, got_outer, got_inner, table, cut_exponent.reshape(1, blocks_z), group_map.reshape(1, blocks_z))
    )
    n_first, n_second = lax.axis_size(FIRST), lax.axis_size(SECOND)
    scale = 1.0 / (nx * ny * (size // blocks_z))
    final = pl.pallas_call(
        functools.partial(final_kernel, nx, ny, scale),
        out_shape=(in_vmem((nx * ny, size)), in_vmem((n_first, 1, 128))),
        in_specs=[VMEM] * 6,
        out_specs=(VMEM, VMEM),
        input_output_aliases={5: 0},
        scratch_shapes=[pltpu.VMEM((4, 8, size), F32)],
        compiler_params=PARAMS,
        name="final",
    )
    coeffs, mass = final(*near(outer, inner, acc, limits, hot, base))
    spread = pl.pallas_call(
        spread_kernel,
        out_shape=in_vmem((n_second, 1, 128)),
        in_specs=[VMEM],
        out_specs=VMEM,
        compiler_params=PARAMS,
        name="spread",
    )
    mass = spread(*near(lax.all_to_all(mass, FIRST, 0, 0)))
    mass = lax.all_to_all(mass, SECOND, 0, 0).sum(0)
    return coeffs.reshape(nx, ny, size), mass[0, : 4 * GROUPS].reshape(4, GROUPS).T


def solution(mesh):
    rows, cols = mesh.devices.shape
    z, y_hi = rows // 2, max(cols // 8, 1)
    devices = mesh.devices.reshape(z, 2, y_hi, cols // 2 // y_hi, 2)
    split = P(ROW, COL, None)
    return jax.shard_map(
        shards,
        mesh=Mesh(devices, ROW + COL),
        in_specs=(split, split, split),
        out_specs=(split, P()),
        check_vma=False,
    )
```

```python
import functools

import jax
import jax.numpy as jnp
import numpy as np
from jax import lax
from jax.experimental import pallas as pl
from jax.experimental.pallas import tpu as pltpu
from jax.sharding import Mesh
from jax.sharding import PartitionSpec as P

GROUPS = 16
ROW = ("z", "y_lo")
COL = ("y_hi", "x", "core")
FIRST = ("y_hi", "y_lo", "core")
SECOND = ("z", "x")
LEVELS = (0.25, 0.5, 1.0, 2.0)
A, B, C, G = 0.5625, 0.0625, 0.28125, 0.03125
F32 = jnp.float32
VMEM = pl.BlockSpec(memory_space=pltpu.VMEM)
PARAMS = pltpu.CompilerParams(vmem_limit_bytes=16 << 20)
ANY = pl.BlockSpec(memory_space=pl.ANY)


def in_vmem(shape, dtype=F32):
    return pltpu.VMEM(shape, dtype)


def lane_lift(v):
    size = v.shape[-1]
    odd = lax.broadcasted_iota(jnp.int32, v.shape, 1) % 2 == 1
    near = pltpu.roll(v, 1, axis=1) + pltpu.roll(v, size - 1, axis=1)
    far = pltpu.roll(v, 3, axis=1) + pltpu.roll(v, size - 3, axis=1)
    w = jnp.where(odd, v - (A * near - B * far), v)
    near = pltpu.roll(w, 1, axis=1) + pltpu.roll(w, size - 1, axis=1)
    far = pltpu.roll(w, 3, axis=1) + pltpu.roll(w, size - 3, axis=1)
    return jnp.where(odd, w, w + (C * near - G * far))


def lane_table(size):
    shift = lambda m, by: np.roll(m, by, axis=1)
    ident = np.eye(size)
    e, o = ident[:, 0::2], ident[:, 1::2]
    d = o - A * (e + shift(e, -1)) + B * (shift(e, 1) + shift(e, -2))
    s = e + C * (shift(d, 1) + d) - G * (shift(d, 2) + shift(d, -1))
    return np.stack([s, d], axis=2).reshape(size, size).astype(jnp.bfloat16)


def table_lift(v, table, pieces=2):
    total = None
    for _ in range(pieces):
        piece = v.astype(jnp.bfloat16)
        v = v - piece.astype(F32)
        term = jnp.dot(piece, table, preferred_element_type=F32)
        total = term if total is None else total + term
    return total


def to_right(at):
    e0, o0, e1, o1, e2 = at(2), at(1), at(4), at(3), at(6)
    return e0, o0 - A * e0 + B * e1, o1 - A * (e1 + e0) + B * e2


def to_left(at):
    e0, o0, e1, e2 = at(0), at(1), at(2), at(4)
    return e0, e1, o0 - A * (e0 + e1) + B * e2


FROM_LEFT = {0: (C * B, C, -G), 1: (B, 0.0, 0.0), 2: (C * B, -G, 0.0), 4: (-G * B, 0.0, 0.0)}
FROM_RIGHT = {
    6: (-G * B, 0.0, 0.0),
    4: (C * B + G * A, -G * B, 0.0),
    3: (B, 0.0, 0.0),
    2: (C * (B - A), C * B, -G),
    1: (-A, B, 0.0),
}


def combine(coefs, lines):
    total = None
    for coef, line in zip(coefs, lines):
        if coef != 0.0:
            term = coef * line
            total = term if total is None else total + term
    return total


def edge_kernel(nx, ny, p_ref, right_ref, left_ref, first, last, sems):
    lo = pltpu.make_async_copy(p_ref.at[pl.ds(0, 5 * ny)], first, sems.at[0])
    hi = pltpu.make_async_copy(p_ref.at[pl.ds((nx - 6) * ny, 6 * ny)], last, sems.at[1])
    lo.start()
    hi.start()
    lo.wait()
    for k, v in enumerate(to_left(lambda i: first[pl.ds(i * ny, ny), :])):
        left_ref[pl.ds(k * ny, ny), :] = v
    hi.wait()
    for k, v in enumerate(to_right(lambda i: last[pl.ds((6 - i) * ny, ny), :])):
        right_ref[pl.ds(k * ny, ny), :] = v


def boundary_lines(head, tail):
    return (*to_right(lambda i: tail[8 - i : 9 - i, :]), *to_left(lambda i: head[i : i + 1, :]))


def edge_weights(size):
    row = lax.broadcasted_iota(jnp.int32, (8, size), 0)

    def weights(table, place, k):
        total = jnp.zeros((8, size), F32)
        for line, coefs in table.items():
            if coefs[k] != 0.0:
                total = jnp.where(row == place(line), coefs[k], total)
        return total

    head = [weights(FROM_LEFT, lambda i: i, k) for k in range(3)]
    return head, [weights(FROM_RIGHT, lambda i: 8 - i, k) for k in range(3)]


def bulk_kernel(nx, ny, p_ref, table_hbm, w_ref, inner_ref, outer_ref, table_ref, sem):
    copy = pltpu.make_async_copy(table_hbm, table_ref, sem)
    copy.start()
    half = nx // 2
    tiles = w_ref.shape[1] // 128

    def column(i, _):
        lanes = pl.ds(pl.multiple_of(i % tiles * 128, 128), 128)
        rows = lambda x: pl.ds(pl.multiple_of(x * ny + i // tiles * 8, 8), 8)
        e = [p_ref[rows(2 * j), lanes] for j in range(half)]
        d = {-2: B * e[0], -1: B * e[1] - A * e[0], half: B * e[half - 1]}
        for j in range(half):
            near = e[j] + e[j + 1] if j + 1 < half else e[j]
            v = p_ref[rows(2 * j + 1), lanes] - A * near
            far = [e[i] for i in (j - 1, j + 2) if 0 <= i < half]
            if far:
                v = v + B * functools.reduce(lambda a, b: a + b, far)
            d[j] = v
            w_ref[rows(2 * j + 1), lanes] = v
        for j in range(half):
            w_ref[rows(2 * j), lanes] = e[j] + (C * (d[j - 1] + d[j]) - G * (d[j - 2] + d[j + 1]))
        return 0

    lax.fori_loop(0, ny // 8 * tiles, column, 0, unroll=2)
    copy.wait()
    size = nx * ny // 4
    for i in range(4):
        part = pl.ds(i * size, size)
        w_ref[part, :] = table_lift(w_ref[part, :], table_ref[...], 3)
    even = lax.axis_index("core") == 0

    def partial(x, _):
        head = w_ref[pl.ds(pl.multiple_of(x * ny, 8), 8), :]
        tail = w_ref[pl.ds(pl.multiple_of(x * ny + ny - 8, 8), 8), :]
        lines = boundary_lines(head, tail)
        for k, (right, left) in enumerate(zip(lines[:3], lines[3:])):
            inner_ref[pl.ds(k * nx + x, 1), :] = jnp.where(even, right, left)
            outer_ref[pl.ds(k * nx + x, 1), :] = jnp.where(even, left, right)
        return 0

    lax.fori_loop(0, nx, partial, 0, unroll=8)


def plane_kernel(nx, ny, got_l_ref, got_r_ref, table_ref, inner_in, outer_in, inner_ref, outer_ref, lines):
    size = table_ref.shape[0]
    even = lax.axis_index("core") == 0
    lines[...] = jnp.zeros_like(lines)
    for h in range(6):
        got = (got_l_ref, got_r_ref)[h // 3]
        at = h % 3 * ny
        for m, line in enumerate(boundary_lines(got[at : at + 8, :], got[at + ny - 8 : at + ny, :])):
            lines[6 * h + m : 6 * h + m + 1, :] = line
    lines[...] = table_lift(lines[...], table_ref[...])
    inner_ref[...] = inner_in[...]
    outer_ref[...] = outer_in[...]
    for first, at, weights in zip((0, 3), (0, nx - 8), edge_weights(size)):
        for k in range(3):
            row = lambda h, m: lines[6 * h + m : 6 * h + m + 1, :]
            right = sum(weights[i] * row(first + i, k) for i in range(3))
            left = sum(weights[i] * row(first + i, 3 + k) for i in range(3))
            part = slice(k * nx + at, k * nx + at + 8)
            inner_ref[part, :] = inner_ref[part, :] + jnp.where(even, right, left)
            outer_ref[part, :] = outer_ref[part, :] + jnp.where(even, left, right)


def excess(acc, v, even_plane, limits):
    m = jnp.abs(v)
    if even_plane:
        row = lax.broadcasted_iota(jnp.int32, v.shape, 0)
        lane = lax.broadcasted_iota(jnp.int32, v.shape, 1)
        m = jnp.where((row | lane) % 2 == 1, m, 0.0)
    return [a + jnp.maximum(m - lim, 0.0) for a, lim in zip(acc, limits)]


def rows_kernel(nx, ny, w_ref, got_l_ref, got_r_ref, table_ref, cut_ref, group_ref, out_ref, acc_ref, lim_ref, hot_ref, halo, fixed_ref):
    size = w_ref.shape[1]
    blocks = cut_ref.shape[1]
    lane = lax.broadcasted_iota(jnp.int32, (1, size), 1)
    cut = jnp.zeros((1, size), jnp.int32)
    place = lax.broadcasted_iota(jnp.int32, (8, 128), 0)
    group = jnp.zeros((8, 128), jnp.int32)
    for c in range(blocks):
        cut = jnp.where(lane // (size // blocks) == c, cut_ref[:, c : c + 1], cut)
        group = jnp.where(place // 4 == c, group_ref[:, c : c + 1], group)
    scales = jnp.exp2(-cut.astype(F32))
    for l, level in enumerate(LEVELS):
        lim_ref[l : l + 1, :] = level * scales
    hot = lax.broadcasted_iota(jnp.int32, (8, 128), 1) == GROUPS * (place % 4) + group
    hot_ref[...] = jnp.where(hot, 1.0, 0.0)
    acc_ref[...] = jnp.zeros_like(acc_ref)

    halo[pl.ds(0, 3 * ny), :] = table_lift(got_l_ref[...], table_ref[...])
    halo[pl.ds(3 * ny, 3 * ny), :] = table_lift(got_r_ref[...], table_ref[...])

    def fix(t, _):
        rows = lambda x: pl.ds(pl.multiple_of(x * ny + t * 8, 8), 8)
        lines = [halo[rows(k), :] for k in range(3)]
        for x in range(6):
            v = w_ref[rows(x), :]
            fixed_ref[rows(x), :] = v + combine(FROM_LEFT[x], lines) if x in FROM_LEFT else v
        lines = [halo[rows(3 + k), :] for k in range(3)]
        for back in range(6, 0, -1):
            v = w_ref[rows(nx - back), :]
            fixed_ref[rows(12 - back), :] = v + combine(FROM_RIGHT[back], lines) if back in FROM_RIGHT else v
        return 0

    lax.fori_loop(0, ny // 8, fix, 0)

    def lift(src, at_plane):
        v = src[pl.ds(pl.multiple_of(at_plane * ny, 8), ny), :]
        v = jnp.concatenate([v, jnp.zeros((8, size), F32)], axis=0)
        odd = lax.broadcasted_iota(jnp.int32, v.shape, 0) % 2 == 1
        at = lambda u, by: pltpu.roll(u, by % (ny + 8), axis=0)
        w = jnp.where(odd, v - (A * (at(v, 1) + at(v, -1)) - B * (at(v, 3) + at(v, -3))), v)
        s = w + (C * (at(w, 1) + at(w, -1)) - G * (at(w, 3) + at(w, -3)))
        return jnp.where(odd, w, s)[0:ny, :]

    def plane(src, at_plane, x, even_plane):
        v = lift(src, at_plane)
        out_ref[pl.ds(pl.multiple_of(x * ny, 8), ny), :] = v
        limits = [jnp.broadcast_to(lim_ref[l : l + 1, :], (8, size)) for l in range(4)]
        acc = [acc_ref[l] for l in range(4)]
        for t in range(1, ny // 8 - 1):
            acc = excess(acc, v[8 * t : 8 * t + 8, :], even_plane, limits)
        for l in range(4):
            acc_ref[l] = acc[l]

    for src, start, x0, each in ((fixed_ref, 0, 0, 6), (w_ref, 6, 6, nx - 12), (fixed_ref, 6, nx - 6, 6)):

        def pair(j, _):
            plane(src, start + 2 * j, x0 + 2 * j, True)
            plane(src, start + 2 * j + 1, x0 + 2 * j + 1, False)
            return 0

        lax.fori_loop(0, each // 2, pair, 0)


def final_kernel(nx, ny, scale, outer_ref, inner_ref, acc_in, lim_ref, hot_ref, base_ref, out_ref, mass_ref, acc_ref):
    size = base_ref.shape[1]
    from_l, from_r = edge_weights(size)
    acc_ref[...] = acc_in[...]
    even = lax.axis_index("core") == 0

    def tiles(x, even_plane):
        limits = [jnp.broadcast_to(lim_ref[l : l + 1, :], (8, size)) for l in range(4)]
        acc = [acc_ref[l] for l in range(4)]
        inner = [inner_ref[pl.ds(k * nx + x, 1), :] for k in range(3)]
        outer = [outer_ref[pl.ds(k * nx + x, 1), :] for k in range(3)]
        left = [jnp.where(even, o, i) for i, o in zip(inner, outer)]
        right = [jnp.where(even, i, o) for i, o in zip(inner, outer)]
        for got, table, at in ((left, from_l, 0), (right, from_r, ny - 8)):
            part = pl.ds(pl.multiple_of(x * ny + at, 8), 8)
            v = base_ref[part, :]
            for k in range(3):
                v = v + table[k] * got[k]
            out_ref[part, :] = v
            acc = excess(acc, v, even_plane, limits)
        for l in range(4):
            acc_ref[l] = acc[l]

    def pair(j, _):
        tiles(2 * j, True)
        tiles(2 * j + 1, False)
        return 0

    lax.fori_loop(0, nx // 2, pair, 0, unroll=2)
    blocks = 2
    width = size // blocks
    lines = []
    for c in range(blocks):
        for l in range(4):
            lines.append(jnp.sum(acc_ref[l, :, c * width : (c + 1) * width], axis=0, keepdims=True))
    sums = jnp.sum(jnp.concatenate(lines, axis=0), axis=1, keepdims=True)
    line = jnp.sum((sums * scale) * hot_ref[...], axis=0, keepdims=True)
    for i in range(mass_ref.shape[0]):
        mass_ref[i] = line


def spread_kernel(parts_ref, out_ref):
    total = parts_ref[0]
    for i in range(1, parts_ref.shape[0]):
        total = total + parts_ref[i]
    for i in range(out_ref.shape[0]):
        out_ref[i] = total


def pair_swaps(n):
    inner = [(i, i ^ 1) for i in range(n)]
    return inner, [((i + 1) % n, (j + 1) % n) for i, j in inner]


def shift(value, by, axes):
    n = lax.axis_size(axes)
    return lax.ppermute(value, axes, [(i, (i + by) % n) for i in range(n)])


def exchange(outer, inner, axes):
    swap_inner, swap_outer = pair_swaps(lax.axis_size(axes))
    inner = lax.ppermute(inner, axes, swap_inner)
    return lax.ppermute(outer, axes, swap_outer), inner


def near(*values):
    return [pltpu.with_memory_space_constraint(v, pltpu.VMEM) for v in values]


def far(value):
    return pltpu.with_memory_space_constraint(value, pltpu.HBM)


def cost(flops):
    return pl.CostEstimate(flops=flops, bytes_accessed=4 << 20, transcendentals=0)


def shards(pressure, cut_exponent, group_map):
    nx, ny, size = pressure.shape
    flat = pressure.reshape(nx * ny, size)
    blocks_z = cut_exponent.shape[2]
    table = jnp.asarray(lane_table(size))
    edge = pl.pallas_call(
        functools.partial(edge_kernel, nx, ny),
        out_shape=(in_vmem((3 * ny, size)), in_vmem((3 * ny, size))),
        in_specs=[ANY],
        out_specs=(VMEM, VMEM),
        scratch_shapes=[pltpu.VMEM((5 * ny, size), F32), pltpu.VMEM((6 * ny, size), F32), pltpu.SemaphoreType.DMA((2,))],
        compiler_params=PARAMS,
        name="edge",
    )
    right, left = edge(far(flat))
    later, right, left = lax.optimization_barrier((flat, right, left))
    from_left, from_right = shift(right, 1, ROW), shift(left, -1, ROW)
    bulk = pl.pallas_call(
        functools.partial(bulk_kernel, nx, ny),
        out_shape=(
            in_vmem((nx * ny, size)),
            in_vmem((3 * nx, size)),
            in_vmem((3 * nx, size)),
            in_vmem((size, size), jnp.bfloat16),
        ),
        in_specs=[VMEM, ANY],
        out_specs=(VMEM,) * 4,
        scratch_shapes=[pltpu.SemaphoreType.DMA],
        cost_estimate=cost(40_000_000),
        compiler_params=PARAMS,
        name="bulk",
    )
    work, inner, outer, table = bulk(*near(later), far(table))
    plane = pl.pallas_call(
        functools.partial(plane_kernel, nx, ny),
        out_shape=(in_vmem((3 * nx, size)), in_vmem((3 * nx, size))),
        in_specs=[VMEM] * 5,
        out_specs=(VMEM, VMEM),
        scratch_shapes=[pltpu.VMEM((40, size), F32)],
        compiler_params=PARAMS,
        name="plane",
    )
    inner, outer = plane(*near(from_left, from_right, table, inner, outer))
    outer, inner = exchange(outer, inner, COL)
    rows = pl.pallas_call(
        functools.partial(rows_kernel, nx, ny),
        out_shape=(in_vmem((nx * ny, size)), in_vmem((4, 8, size)), in_vmem((4, size)), in_vmem((8, 128))),
        in_specs=[VMEM] * 6,
        out_specs=(VMEM,) * 4,
        scratch_shapes=[pltpu.VMEM((6 * ny, size), F32), pltpu.VMEM((12 * ny, size), F32)],
        cost_estimate=cost(40_000_000),
        compiler_params=PARAMS,
        name="rows",
    )
    base, acc, limits, hot = rows(
        *near(work, from_left, from_right, table, cut_exponent.reshape(1, blocks_z), group_map.reshape(1, blocks_z))
    )
    n_first, n_second = lax.axis_size(FIRST), lax.axis_size(SECOND)
    scale = 1.0 / (nx * ny * (size // blocks_z))
    final = pl.pallas_call(
        functools.partial(final_kernel, nx, ny, scale),
        out_shape=(in_vmem((nx * ny, size)), in_vmem((n_first, 1, 128))),
        in_specs=[VMEM] * 6,
        out_specs=(VMEM, VMEM),
        input_output_aliases={5: 0},
        scratch_shapes=[pltpu.VMEM((4, 8, size), F32)],
        compiler_params=PARAMS,
        name="final",
    )
    coeffs, mass = final(*near(outer, inner, acc, limits, hot, base))
    spread = pl.pallas_call(
        spread_kernel,
        out_shape=in_vmem((n_second, 1, 128)),
        in_specs=[VMEM],
        out_specs=VMEM,
        compiler_params=PARAMS,
        name="spread",
    )
    mass = spread(*near(lax.all_to_all(mass, FIRST, 0, 0)))
    mass = lax.all_to_all(mass, SECOND, 0, 0).sum(0)
    return coeffs.reshape(nx, ny, size), mass[0, : 4 * GROUPS].reshape(4, GROUPS).T


def solution(mesh):
    rows, cols = mesh.devices.shape
    z, y_hi = rows // 2, max(cols // 8, 1)
    devices = mesh.devices.reshape(z, 2, y_hi, cols // 2 // y_hi, 2)
    split = P(ROW, COL, None)
    return jax.shard_map(
        shards,
        mesh=Mesh(devices, ROW + COL),
        in_specs=(split, split, split),
        out_specs=(split, P()),
        check_vma=False,
    )
```

```python
import functools

import jax
import jax.numpy as jnp
import numpy as np
from jax import lax
from jax.experimental import pallas as pl
from jax.experimental.pallas import tpu as pltpu
from jax.sharding import Mesh
from jax.sharding import PartitionSpec as P

GROUPS = 16
ROW = ("z", "y_lo")
COL = ("y_hi", "x", "core")
FIRST = ("z", "core")
SECOND = ("y_hi", "y_lo", "x")
LEVELS = (0.25, 0.5, 1.0, 2.0)
A, B, C, G = 0.5625, 0.0625, 0.28125, 0.03125
F32 = jnp.float32
VMEM = pl.BlockSpec(memory_space=pltpu.VMEM)
PARAMS = pltpu.CompilerParams(vmem_limit_bytes=16 << 20)
ANY = pl.BlockSpec(memory_space=pl.ANY)


def in_vmem(shape, dtype=F32):
    return pltpu.VMEM(shape, dtype)


def lane_lift(v):
    size = v.shape[-1]
    odd = lax.broadcasted_iota(jnp.int32, v.shape, 1) % 2 == 1
    near = pltpu.roll(v, 1, axis=1) + pltpu.roll(v, size - 1, axis=1)
    far = pltpu.roll(v, 3, axis=1) + pltpu.roll(v, size - 3, axis=1)
    w = jnp.where(odd, v - (A * near - B * far), v)
    near = pltpu.roll(w, 1, axis=1) + pltpu.roll(w, size - 1, axis=1)
    far = pltpu.roll(w, 3, axis=1) + pltpu.roll(w, size - 3, axis=1)
    return jnp.where(odd, w, w + (C * near - G * far))


def lane_table(size):
    shift = lambda m, by: np.roll(m, by, axis=1)
    ident = np.eye(size)
    e, o = ident[:, 0::2], ident[:, 1::2]
    d = o - A * (e + shift(e, -1)) + B * (shift(e, 1) + shift(e, -2))
    s = e + C * (shift(d, 1) + d) - G * (shift(d, 2) + shift(d, -1))
    return np.stack([s, d], axis=2).reshape(size, size).astype(jnp.bfloat16)


def table_lift(v, table, pieces=2):
    total = None
    for _ in range(pieces):
        piece = v.astype(jnp.bfloat16)
        v = v - piece.astype(F32)
        term = jnp.dot(piece, table, preferred_element_type=F32)
        total = term if total is None else total + term
    return total


def to_right(at):
    e0, o0, e1, o1, e2 = at(2), at(1), at(4), at(3), at(6)
    return e0, o0 - A * e0 + B * e1, o1 - A * (e1 + e0) + B * e2


def to_left(at):
    e0, o0, e1, e2 = at(0), at(1), at(2), at(4)
    return e0, e1, o0 - A * (e0 + e1) + B * e2


FROM_LEFT = {0: (C * B, C, -G), 1: (B, 0.0, 0.0), 2: (C * B, -G, 0.0), 4: (-G * B, 0.0, 0.0)}
FROM_RIGHT = {
    6: (-G * B, 0.0, 0.0),
    4: (C * B + G * A, -G * B, 0.0),
    3: (B, 0.0, 0.0),
    2: (C * (B - A), C * B, -G),
    1: (-A, B, 0.0),
}


def combine(coefs, lines):
    total = None
    for coef, line in zip(coefs, lines):
        if coef != 0.0:
            term = coef * line
            total = term if total is None else total + term
    return total


def edge_kernel(nx, ny, p_ref, outer_ref, inner_ref, first, last, sems):
    lo = pltpu.make_async_copy(p_ref.at[pl.ds(0, 5 * ny)], first, sems.at[0])
    hi = pltpu.make_async_copy(p_ref.at[pl.ds((nx - 6) * ny, 6 * ny)], last, sems.at[1])
    lo.start()
    hi.start()
    even = lax.axis_index("y_lo") == 0
    lo.wait()
    hi.wait()
    left = to_left(lambda i: first[pl.ds(i * ny, ny), :])
    right = to_right(lambda i: last[pl.ds((6 - i) * ny, ny), :])
    for k, (r, l) in enumerate(zip(right, left)):
        outer_ref[pl.ds(k * ny, ny), :] = jnp.where(even, l, r)
        inner_ref[pl.ds(k * ny, ny), :] = jnp.where(even, r, l)


def boundary_lines(head, tail):
    return (*to_right(lambda i: tail[8 - i : 9 - i, :]), *to_left(lambda i: head[i : i + 1, :]))


def edge_weights(size):
    row = lax.broadcasted_iota(jnp.int32, (8, size), 0)

    def weights(table, place, k):
        total = jnp.zeros((8, size), F32)
        for line, coefs in table.items():
            if coefs[k] != 0.0:
                total = jnp.where(row == place(line), coefs[k], total)
        return total

    head = [weights(FROM_LEFT, lambda i: i, k) for k in range(3)]
    return head, [weights(FROM_RIGHT, lambda i: 8 - i, k) for k in range(3)]


def bulk_kernel(nx, ny, p_ref, table_hbm, w_ref, inner_ref, outer_ref, table_ref, sem):
    copy = pltpu.make_async_copy(table_hbm, table_ref, sem)
    copy.start()
    half = nx // 2
    tiles = w_ref.shape[1] // 128

    def column(i, _):
        lanes = pl.ds(pl.multiple_of(i % tiles * 128, 128), 128)
        rows = lambda x: pl.ds(pl.multiple_of(x * ny + i // tiles * 8, 8), 8)
        e = [p_ref[rows(2 * j), lanes] for j in range(half)]
        d = {-2: B * e[0], -1: B * e[1] - A * e[0], half: B * e[half - 1]}
        for j in range(half):
            near = e[j] + e[j + 1] if j + 1 < half else e[j]
            v = p_ref[rows(2 * j + 1), lanes] - A * near
            far = [e[i] for i in (j - 1, j + 2) if 0 <= i < half]
            if far:
                v = v + B * functools.reduce(lambda a, b: a + b, far)
            d[j] = v
            w_ref[rows(2 * j + 1), lanes] = v
        for j in range(half):
            w_ref[rows(2 * j), lanes] = e[j] + (C * (d[j - 1] + d[j]) - G * (d[j - 2] + d[j + 1]))
        return 0

    lax.fori_loop(0, ny // 8 * tiles, column, 0, unroll=2)
    copy.wait()
    size = nx * ny // 4
    for i in range(4):
        part = pl.ds(i * size, size)
        w_ref[part, :] = table_lift(w_ref[part, :], table_ref[...], 3)
    even = lax.axis_index("core") == 0

    def partial(x, _):
        head = w_ref[pl.ds(pl.multiple_of(x * ny, 8), 8), :]
        tail = w_ref[pl.ds(pl.multiple_of(x * ny + ny - 8, 8), 8), :]
        lines = boundary_lines(head, tail)
        for k, (right, left) in enumerate(zip(lines[:3], lines[3:])):
            inner_ref[pl.ds(k * nx + x, 1), :] = jnp.where(even, right, left)
            outer_ref[pl.ds(k * nx + x, 1), :] = jnp.where(even, left, right)
        return 0

    lax.fori_loop(0, nx, partial, 0, unroll=8)


def plane_kernel(nx, ny, got_o_ref, got_i_ref, table_ref, inner_in, outer_in, inner_ref, outer_ref, lines):
    size = table_ref.shape[0]
    even = lax.axis_index("core") == 0
    lines[...] = jnp.zeros_like(lines)
    y_even = lax.axis_index("y_lo") == 0
    for h in range(6):
        at = h % 3 * ny
        of_even, of_odd = (got_o_ref, got_i_ref) if h < 3 else (got_i_ref, got_o_ref)
        got = lambda part: jnp.where(y_even, of_even[part, :], of_odd[part, :])
        for m, line in enumerate(boundary_lines(got(slice(at, at + 8)), got(slice(at + ny - 8, at + ny)))):
            lines[6 * h + m : 6 * h + m + 1, :] = line
    lines[...] = table_lift(lines[...], table_ref[...])
    inner_ref[...] = inner_in[...]
    outer_ref[...] = outer_in[...]
    for first, at, weights in zip((0, 3), (0, nx - 8), edge_weights(size)):
        for k in range(3):
            row = lambda h, m: lines[6 * h + m : 6 * h + m + 1, :]
            right = sum(weights[i] * row(first + i, k) for i in range(3))
            left = sum(weights[i] * row(first + i, 3 + k) for i in range(3))
            part = slice(k * nx + at, k * nx + at + 8)
            inner_ref[part, :] = inner_ref[part, :] + jnp.where(even, right, left)
            outer_ref[part, :] = outer_ref[part, :] + jnp.where(even, left, right)


def excess(acc, v, even_plane, limits):
    m = jnp.abs(v)
    if even_plane:
        row = lax.broadcasted_iota(jnp.int32, v.shape, 0)
        lane = lax.broadcasted_iota(jnp.int32, v.shape, 1)
        m = jnp.where((row | lane) % 2 == 1, m, 0.0)
    return [a + jnp.maximum(m - lim, 0.0) for a, lim in zip(acc, limits)]


def rows_kernel(nx, ny, w_ref, got_o_ref, got_i_ref, table_ref, cut_ref, group_ref, out_ref, edge_ref, acc_ref, lim_ref, hot_ref, halo, fixed_ref, mid, sems):
    size = w_ref.shape[1]
    blocks = cut_ref.shape[1]
    lane = lax.broadcasted_iota(jnp.int32, (1, size), 1)
    cut = jnp.zeros((1, size), jnp.int32)
    place = lax.broadcasted_iota(jnp.int32, (8, 128), 0)
    group = jnp.zeros((8, 128), jnp.int32)
    for c in range(blocks):
        cut = jnp.where(lane // (size // blocks) == c, cut_ref[:, c : c + 1], cut)
        group = jnp.where(place // 4 == c, group_ref[:, c : c + 1], group)
    scales = jnp.exp2(-cut.astype(F32))
    for l, level in enumerate(LEVELS):
        lim_ref[l : l + 1, :] = level * scales
    hot = lax.broadcasted_iota(jnp.int32, (8, 128), 1) == GROUPS * (place % 4) + group
    hot_ref[...] = jnp.where(hot, 1.0, 0.0)
    acc_ref[...] = jnp.zeros_like(acc_ref)

    y_even = lax.axis_index("y_lo") == 0
    halo[pl.ds(0, 3 * ny), :] = table_lift(jnp.where(y_even, got_o_ref[...], got_i_ref[...]), table_ref[...])
    halo[pl.ds(3 * ny, 3 * ny), :] = table_lift(jnp.where(y_even, got_i_ref[...], got_o_ref[...]), table_ref[...])

    def fix(t, _):
        rows = lambda x: pl.ds(pl.multiple_of(x * ny + t * 8, 8), 8)
        lines = [halo[rows(k), :] for k in range(3)]
        for x in range(6):
            v = w_ref[rows(x), :]
            fixed_ref[rows(x), :] = v + combine(FROM_LEFT[x], lines) if x in FROM_LEFT else v
        lines = [halo[rows(3 + k), :] for k in range(3)]
        for back in range(6, 0, -1):
            v = w_ref[rows(nx - back), :]
            fixed_ref[rows(12 - back), :] = v + combine(FROM_RIGHT[back], lines) if back in FROM_RIGHT else v
        return 0

    lax.fori_loop(0, ny // 8, fix, 0)

    def lift(src, at_plane):
        v = src[pl.ds(pl.multiple_of(at_plane * ny, 8), ny), :]
        v = jnp.concatenate([v, jnp.zeros((8, size), F32)], axis=0)
        odd = lax.broadcasted_iota(jnp.int32, v.shape, 0) % 2 == 1
        at = lambda u, by: pltpu.roll(u, by % (ny + 8), axis=0)
        w = jnp.where(odd, v - (A * (at(v, 1) + at(v, -1)) - B * (at(v, 3) + at(v, -3))), v)
        s = w + (C * (at(w, 1) + at(w, -1)) - G * (at(w, 3) + at(w, -3)))
        return jnp.where(odd, w, s)[0:ny, :]

    def plane(src, at_plane, x, even_plane):
        v = lift(src, at_plane)
        edge_ref[pl.ds(pl.multiple_of(x * 16, 8), 8), :] = v[0:8, :]
        edge_ref[pl.ds(pl.multiple_of(x * 16 + 8, 8), 8), :] = v[ny - 8 : ny, :]
        mid[x] = v[8 : ny - 8, :]
        limits = [jnp.broadcast_to(lim_ref[l : l + 1, :], (8, size)) for l in range(4)]
        acc = [acc_ref[l] for l in range(4)]
        for t in range(1, ny // 8 - 1):
            acc = excess(acc, v[8 * t : 8 * t + 8, :], even_plane, limits)
        for l in range(4):
            acc_ref[l] = acc[l]

    copies = []
    middle = (nx - 12) // 2
    for n, (src, start, x0, each) in enumerate(
        ((fixed_ref, 0, 0, 6), (w_ref, 6, 6, middle), (w_ref, 6 + middle, 6 + middle, middle), (fixed_ref, 6, nx - 6, 6))
    ):

        def pair(j, _):
            plane(src, start + 2 * j, x0 + 2 * j, True)
            plane(src, start + 2 * j + 1, x0 + 2 * j + 1, False)
            return 0

        lax.fori_loop(0, each // 2, pair, 0)
        part = pl.ds(x0, each)
        copies.append(pltpu.make_async_copy(mid.at[part], out_ref.at[part, pl.ds(8, ny - 16), :], sems.at[n]))
        copies[-1].start()
    for copy in copies:
        copy.wait()


def final_kernel(nx, ny, scale, outer_ref, inner_ref, acc_in, lim_ref, hot_ref, base_ref, out_in, out_ref, mass_ref, acc_ref, done, sems):
    del out_in
    size = base_ref.shape[1]
    from_l, from_r = edge_weights(size)
    acc_ref[...] = acc_in[...]
    even = lax.axis_index("core") == 0

    def tiles(x, even_plane):
        limits = [jnp.broadcast_to(lim_ref[l : l + 1, :], (8, size)) for l in range(4)]
        acc = [acc_ref[l] for l in range(4)]
        inner = [inner_ref[pl.ds(k * nx + x, 1), :] for k in range(3)]
        outer = [outer_ref[pl.ds(k * nx + x, 1), :] for k in range(3)]
        left = [jnp.where(even, o, i) for i, o in zip(inner, outer)]
        right = [jnp.where(even, i, o) for i, o in zip(inner, outer)]
        for n, got, table in ((0, left, from_l), (1, right, from_r)):
            v = base_ref[pl.ds(pl.multiple_of(x * 16 + 8 * n, 8), 8), :]
            for k in range(3):
                v = v + table[k] * got[k]
            done[n, x] = v
            acc = excess(acc, v, even_plane, limits)
        for l in range(4):
            acc_ref[l] = acc[l]

    def pair(j, _):
        tiles(2 * j, True)
        tiles(2 * j + 1, False)
        return 0

    copies = []
    start = 0
    for i, stop in enumerate((nx // 4, nx // 2, 3 * nx // 4, nx - 4, nx)):
        lax.fori_loop(start // 2, stop // 2, pair, 0, unroll=2)
        part = pl.ds(start, stop - start)
        for n, at in enumerate((0, ny - 8)):
            copies.append(pltpu.make_async_copy(done.at[n, part], out_ref.at[part, pl.ds(at, 8), :], sems.at[2 * i + n]))
            copies[-1].start()
        start = stop
    blocks = 2
    width = size // blocks
    lines = []
    for c in range(blocks):
        for l in range(4):
            lines.append(jnp.sum(acc_ref[l, :, c * width : (c + 1) * width], axis=0, keepdims=True))
    sums = jnp.sum(jnp.concatenate(lines, axis=0), axis=1, keepdims=True)
    line = jnp.sum((sums * scale) * hot_ref[...], axis=0, keepdims=True)
    for i in range(mass_ref.shape[0]):
        mass_ref[i] = line
    for copy in copies:
        copy.wait()


def spread_kernel(parts_ref, out_ref):
    total = parts_ref[0]
    for i in range(1, parts_ref.shape[0]):
        total = total + parts_ref[i]
    for i in range(out_ref.shape[0]):
        out_ref[i] = total


def pair_swaps(n):
    inner = [(i, i ^ 1) for i in range(n)]
    return inner, [((i + 1) % n, (j + 1) % n) for i, j in inner]


def exchange(outer, inner, axes):
    swap_inner, swap_outer = pair_swaps(lax.axis_size(axes))
    inner = lax.ppermute(inner, axes, swap_inner)
    return lax.ppermute(outer, axes, swap_outer), inner


def near(*values):
    return [pltpu.with_memory_space_constraint(v, pltpu.VMEM) for v in values]


def far(value):
    return pltpu.with_memory_space_constraint(value, pltpu.HBM)


def cost(flops):
    return pl.CostEstimate(flops=flops, bytes_accessed=4 << 20, transcendentals=0)


def shards(pressure, cut_exponent, group_map):
    nx, ny, size = pressure.shape
    flat = pressure.reshape(nx * ny, size)
    blocks_z = cut_exponent.shape[2]
    table = jnp.asarray(lane_table(size))
    edge = pl.pallas_call(
        functools.partial(edge_kernel, nx, ny),
        out_shape=(in_vmem((3 * ny, size)), in_vmem((3 * ny, size))),
        in_specs=[ANY],
        out_specs=(VMEM, VMEM),
        scratch_shapes=[pltpu.VMEM((5 * ny, size), F32), pltpu.VMEM((6 * ny, size), F32), pltpu.SemaphoreType.DMA((2,))],
        compiler_params=PARAMS,
        name="edge",
    )
    outer, inner = edge(far(flat))
    later, outer, inner = lax.optimization_barrier((flat, outer, inner))
    got_outer, got_inner = exchange(outer, inner, ROW)
    bulk = pl.pallas_call(
        functools.partial(bulk_kernel, nx, ny),
        out_shape=(
            in_vmem((nx * ny, size)),
            in_vmem((3 * nx, size)),
            in_vmem((3 * nx, size)),
            in_vmem((size, size), jnp.bfloat16),
        ),
        in_specs=[VMEM, ANY],
        out_specs=(VMEM,) * 4,
        scratch_shapes=[pltpu.SemaphoreType.DMA],
        cost_estimate=cost(40_000_000),
        compiler_params=PARAMS,
        name="bulk",
    )
    work, inner, outer, table = bulk(*near(later), far(table))
    plane = pl.pallas_call(
        functools.partial(plane_kernel, nx, ny),
        out_shape=(in_vmem((3 * nx, size)), in_vmem((3 * nx, size))),
        in_specs=[VMEM] * 5,
        out_specs=(VMEM, VMEM),
        scratch_shapes=[pltpu.VMEM((40, size), F32)],
        compiler_params=PARAMS,
        name="plane",
    )
    inner, outer = plane(*near(got_outer, got_inner, table, inner, outer))
    outer, inner = exchange(outer, inner, COL)
    rows = pl.pallas_call(
        functools.partial(rows_kernel, nx, ny),
        out_shape=(
            jax.ShapeDtypeStruct((nx, ny, size), F32),
            in_vmem((nx * 16, size)),
            in_vmem((4, 8, size)),
            in_vmem((4, size)),
            in_vmem((8, 128)),
        ),
        in_specs=[VMEM] * 6,
        out_specs=(ANY, *(VMEM,) * 4),
        scratch_shapes=[
            pltpu.VMEM((6 * ny, size), F32),
            pltpu.VMEM((12 * ny, size), F32),
            pltpu.VMEM((nx, ny - 16, size), F32),
            pltpu.SemaphoreType.DMA((4,)),
        ],
        cost_estimate=cost(40_000_000),
        compiler_params=PARAMS,
        name="rows",
    )
    coeffs, base, acc, limits, hot = rows(
        *near(work, got_outer, got_inner, table, cut_exponent.reshape(1, blocks_z), group_map.reshape(1, blocks_z))
    )
    n_first, n_second = lax.axis_size(FIRST), lax.axis_size(SECOND)
    scale = 1.0 / (nx * ny * (size // blocks_z))
    final = pl.pallas_call(
        functools.partial(final_kernel, nx, ny, scale),
        out_shape=(jax.ShapeDtypeStruct((nx, ny, size), F32), in_vmem((n_first, 1, 128))),
        in_specs=[VMEM] * 6 + [ANY],
        out_specs=(ANY, VMEM),
        input_output_aliases={6: 0},
        scratch_shapes=[
            pltpu.VMEM((4, 8, size), F32),
            pltpu.VMEM((2, nx, 8, size), F32),
            pltpu.SemaphoreType.DMA((10,)),
        ],
        compiler_params=PARAMS,
        name="final",
    )
    coeffs, mass = final(*near(outer, inner, acc, limits, hot, base), coeffs)
    spread = pl.pallas_call(
        spread_kernel,
        out_shape=in_vmem((n_second, 1, 128)),
        in_specs=[VMEM],
        out_specs=VMEM,
        compiler_params=PARAMS,
        name="spread",
    )
    mass = spread(*near(lax.all_to_all(mass, FIRST, 0, 0)))
    mass = lax.all_to_all(mass, SECOND, 0, 0).sum(0)
    return coeffs, mass[0, : 4 * GROUPS].reshape(4, GROUPS).T


def solution(mesh):
    rows, cols = mesh.devices.shape
    z, y_hi = rows // 2, max(cols // 8, 1)
    devices = mesh.devices.reshape(z, 2, y_hi, cols // 2 // y_hi, 2)
    split = P(ROW, COL, None)
    return jax.shard_map(
        shards,
        mesh=Mesh(devices, ROW + COL),
        in_specs=(split, split, split),
        out_specs=(split, P()),
        check_vma=False,
    )
```

```python
import functools

import jax
import jax.numpy as jnp
import numpy as np
from jax import lax
from jax.experimental import pallas as pl
from jax.experimental.pallas import tpu as pltpu
from jax.sharding import Mesh
from jax.sharding import PartitionSpec as P

GROUPS = 16
ROW = ("z", "y_lo")
COL = ("y_hi", "x", "core")
FIRST = ("z", "core")
SECOND = ("y_hi", "y_lo", "x")
LEVELS = (0.25, 0.5, 1.0, 2.0)
A, B, C, G = 0.5625, 0.0625, 0.28125, 0.03125
F32 = jnp.float32
VMEM = pl.BlockSpec(memory_space=pltpu.VMEM)
PARAMS = pltpu.CompilerParams(vmem_limit_bytes=16 << 20)
ANY = pl.BlockSpec(memory_space=pl.ANY)


def in_vmem(shape, dtype=F32):
    return pltpu.VMEM(shape, dtype)


def lane_table(size):
    shift = lambda m, by: np.roll(m, by, axis=1)
    ident = np.eye(size)
    e, o = ident[:, 0::2], ident[:, 1::2]
    d = o - A * (e + shift(e, -1)) + B * (shift(e, 1) + shift(e, -2))
    s = e + C * (shift(d, 1) + d) - G * (shift(d, 2) + shift(d, -1))
    return np.stack([s, d], axis=2).reshape(size, size).astype(jnp.bfloat16)


def table_lift(v, table, pieces=2):
    total = None
    for _ in range(pieces):
        piece = v.astype(jnp.bfloat16)
        v = v - piece.astype(F32)
        term = jnp.dot(piece, table, preferred_element_type=F32)
        total = term if total is None else total + term
    return total


def to_right(at):
    e0, o0, e1, o1, e2 = at(2), at(1), at(4), at(3), at(6)
    return e0, o0 - A * e0 + B * e1, o1 - A * (e1 + e0) + B * e2


def to_left(at):
    e0, o0, e1, e2 = at(0), at(1), at(2), at(4)
    return e0, e1, o0 - A * (e0 + e1) + B * e2


FROM_LEFT = {0: (C * B, C, -G), 1: (B, 0.0, 0.0), 2: (C * B, -G, 0.0), 4: (-G * B, 0.0, 0.0)}
FROM_RIGHT = {
    6: (-G * B, 0.0, 0.0),
    4: (C * B + G * A, -G * B, 0.0),
    3: (B, 0.0, 0.0),
    2: (C * (B - A), C * B, -G),
    1: (-A, B, 0.0),
}


def combine(coefs, lines):
    total = None
    for coef, line in zip(coefs, lines):
        if coef != 0.0:
            term = coef * line
            total = term if total is None else total + term
    return total


def edge_kernel(nx, ny, p_ref, outer_ref, inner_ref, first, last, sems):
    lo = pltpu.make_async_copy(p_ref.at[pl.ds(0, 5 * ny)], first, sems.at[0])
    hi = pltpu.make_async_copy(p_ref.at[pl.ds((nx - 6) * ny, 6 * ny)], last, sems.at[1])
    lo.start()
    hi.start()
    even = lax.axis_index("y_lo") == 0
    lo.wait()
    hi.wait()
    left = to_left(lambda i: first[pl.ds(i * ny, ny), :])
    right = to_right(lambda i: last[pl.ds((6 - i) * ny, ny), :])
    for k, (r, l) in enumerate(zip(right, left)):
        outer_ref[pl.ds(k * ny, ny), :] = jnp.where(even, l, r)
        inner_ref[pl.ds(k * ny, ny), :] = jnp.where(even, r, l)


def boundary_lines(head, tail):
    return (*to_right(lambda i: tail[8 - i : 9 - i, :]), *to_left(lambda i: head[i : i + 1, :]))


def edge_weights(size):
    row = lax.broadcasted_iota(jnp.int32, (8, size), 0)

    def weights(table, place, k):
        total = jnp.zeros((8, size), F32)
        for line, coefs in table.items():
            if coefs[k] != 0.0:
                total = jnp.where(row == place(line), coefs[k], total)
        return total

    head = [weights(FROM_LEFT, lambda i: i, k) for k in range(3)]
    return head, [weights(FROM_RIGHT, lambda i: 8 - i, k) for k in range(3)]


def bulk_kernel(nx, ny, p_ref, table_hbm, w_ref, inner_ref, outer_ref, table_ref, sem):
    copy = pltpu.make_async_copy(table_hbm, table_ref, sem)
    copy.start()
    half = nx // 2
    tiles = w_ref.shape[1] // 128

    def column(i, _):
        lanes = pl.ds(pl.multiple_of(i % tiles * 128, 128), 128)
        rows = lambda x: pl.ds(pl.multiple_of(x * ny + i // tiles * 8, 8), 8)
        e = [p_ref[rows(2 * j), lanes] for j in range(half)]
        d = {-2: B * e[0], -1: B * e[1] - A * e[0], half: B * e[half - 1]}
        for j in range(half):
            near = e[j] + e[j + 1] if j + 1 < half else e[j]
            v = p_ref[rows(2 * j + 1), lanes] - A * near
            far = [e[i] for i in (j - 1, j + 2) if 0 <= i < half]
            if far:
                v = v + B * functools.reduce(lambda a, b: a + b, far)
            d[j] = v
            w_ref[rows(2 * j + 1), lanes] = v
        for j in range(half):
            w_ref[rows(2 * j), lanes] = e[j] + (C * (d[j - 1] + d[j]) - G * (d[j - 2] + d[j + 1]))
        return 0

    lax.fori_loop(0, ny // 8 * tiles, column, 0, unroll=2)
    copy.wait()
    size = nx * ny // 4
    for i in range(4):
        part = pl.ds(i * size, size)
        w_ref[part, :] = table_lift(w_ref[part, :], table_ref[...], 3)
    even = lax.axis_index("core") == 0

    def partial(x, _):
        head = w_ref[pl.ds(pl.multiple_of(x * ny, 8), 8), :]
        tail = w_ref[pl.ds(pl.multiple_of(x * ny + ny - 8, 8), 8), :]
        lines = boundary_lines(head, tail)
        for k, (right, left) in enumerate(zip(lines[:3], lines[3:])):
            inner_ref[pl.ds(k * nx + x, 1), :] = jnp.where(even, right, left)
            outer_ref[pl.ds(k * nx + x, 1), :] = jnp.where(even, left, right)
        return 0

    lax.fori_loop(0, nx, partial, 0, unroll=8)


def plane_kernel(nx, ny, got_o_ref, got_i_ref, table_ref, inner_in, outer_in, inner_ref, outer_ref, lines):
    size = table_ref.shape[0]
    even = lax.axis_index("core") == 0
    lines[...] = jnp.zeros_like(lines)
    y_even = lax.axis_index("y_lo") == 0
    for h in range(6):
        at = h % 3 * ny
        of_even, of_odd = (got_o_ref, got_i_ref) if h < 3 else (got_i_ref, got_o_ref)
        got = lambda part: jnp.where(y_even, of_even[part, :], of_odd[part, :])
        for m, line in enumerate(boundary_lines(got(slice(at, at + 8)), got(slice(at + ny - 8, at + ny)))):
            lines[6 * h + m : 6 * h + m + 1, :] = line
    lines[...] = table_lift(lines[...], table_ref[...])
    inner_ref[...] = inner_in[...]
    outer_ref[...] = outer_in[...]
    for first, at, weights in zip((0, 3), (0, nx - 8), edge_weights(size)):
        for k in range(3):
            row = lambda h, m: lines[6 * h + m : 6 * h + m + 1, :]
            right = sum(weights[i] * row(first + i, k) for i in range(3))
            left = sum(weights[i] * row(first + i, 3 + k) for i in range(3))
            part = slice(k * nx + at, k * nx + at + 8)
            inner_ref[part, :] = inner_ref[part, :] + jnp.where(even, right, left)
            outer_ref[part, :] = outer_ref[part, :] + jnp.where(even, left, right)


def excess(acc, v, even_plane, limits):
    m = jnp.abs(v)
    if even_plane:
        row = lax.broadcasted_iota(jnp.int32, v.shape, 0)
        lane = lax.broadcasted_iota(jnp.int32, v.shape, 1)
        m = jnp.where((row | lane) % 2 == 1, m, 0.0)
    return [a + jnp.maximum(m - lim, 0.0) for a, lim in zip(acc, limits)]


def rows_kernel(nx, ny, w_ref, got_o_ref, got_i_ref, table_ref, cut_ref, group_ref, out_ref, edge_ref, acc_ref, lim_ref, hot_ref, halo, fixed_ref, mid, sems):
    size = w_ref.shape[1]
    blocks = cut_ref.shape[1]
    lane = lax.broadcasted_iota(jnp.int32, (1, size), 1)
    cut = jnp.zeros((1, size), jnp.int32)
    place = lax.broadcasted_iota(jnp.int32, (8, 128), 0)
    group = jnp.zeros((8, 128), jnp.int32)
    for c in range(blocks):
        cut = jnp.where(lane // (size // blocks) == c, cut_ref[:, c : c + 1], cut)
        group = jnp.where(place // 4 == c, group_ref[:, c : c + 1], group)
    scales = jnp.exp2(-cut.astype(F32))
    for l, level in enumerate(LEVELS):
        lim_ref[l : l + 1, :] = level * scales
    hot = lax.broadcasted_iota(jnp.int32, (8, 128), 1) == GROUPS * (place % 4) + group
    hot_ref[...] = jnp.where(hot, 1.0, 0.0)
    acc_ref[...] = jnp.zeros_like(acc_ref)

    y_even = lax.axis_index("y_lo") == 0
    halo[pl.ds(0, 3 * ny), :] = table_lift(jnp.where(y_even, got_o_ref[...], got_i_ref[...]), table_ref[...])
    halo[pl.ds(3 * ny, 3 * ny), :] = table_lift(jnp.where(y_even, got_i_ref[...], got_o_ref[...]), table_ref[...])

    def fix(t, _):
        rows = lambda x: pl.ds(pl.multiple_of(x * ny + t * 8, 8), 8)
        lines = [halo[rows(k), :] for k in range(3)]
        for x in range(6):
            v = w_ref[rows(x), :]
            fixed_ref[rows(x), :] = v + combine(FROM_LEFT[x], lines) if x in FROM_LEFT else v
        lines = [halo[rows(3 + k), :] for k in range(3)]
        for back in range(6, 0, -1):
            v = w_ref[rows(nx - back), :]
            fixed_ref[rows(12 - back), :] = v + combine(FROM_RIGHT[back], lines) if back in FROM_RIGHT else v
        return 0

    lax.fori_loop(0, ny // 8, fix, 0)

    def lift(src, at_plane):
        v = src[pl.ds(pl.multiple_of(at_plane * ny, 8), ny), :]
        v = jnp.concatenate([v, jnp.zeros((8, size), F32)], axis=0)
        odd = lax.broadcasted_iota(jnp.int32, v.shape, 0) % 2 == 1
        at = lambda u, by: pltpu.roll(u, by % (ny + 8), axis=0)
        w = jnp.where(odd, v - (A * (at(v, 1) + at(v, -1)) - B * (at(v, 3) + at(v, -3))), v)
        s = w + (C * (at(w, 1) + at(w, -1)) - G * (at(w, 3) + at(w, -3)))
        return jnp.where(odd, w, s)[0:ny, :]

    def plane(src, at_plane, x, even_plane):
        v = lift(src, at_plane)
        edge_ref[pl.ds(pl.multiple_of(x * 16, 8), 8), :] = v[0:8, :]
        edge_ref[pl.ds(pl.multiple_of(x * 16 + 8, 8), 8), :] = v[ny - 8 : ny, :]
        mid[x] = v[8 : ny - 8, :]
        limits = [jnp.broadcast_to(lim_ref[l : l + 1, :], (8, size)) for l in range(4)]
        acc = [acc_ref[l] for l in range(4)]
        for t in range(1, ny // 8 - 1):
            acc = excess(acc, v[8 * t : 8 * t + 8, :], even_plane, limits)
        for l in range(4):
            acc_ref[l] = acc[l]

    copies = []
    middle = (nx - 12) // 2
    for n, (src, start, x0, each) in enumerate(
        ((fixed_ref, 0, 0, 6), (w_ref, 6, 6, middle), (w_ref, 6 + middle, 6 + middle, middle), (fixed_ref, 6, nx - 6, 6))
    ):

        def pair(j, _):
            plane(src, start + 2 * j, x0 + 2 * j, True)
            plane(src, start + 2 * j + 1, x0 + 2 * j + 1, False)
            return 0

        lax.fori_loop(0, each // 2, pair, 0)
        part = pl.ds(x0, each)
        copies.append(pltpu.make_async_copy(mid.at[part], out_ref.at[part, pl.ds(8, ny - 16), :], sems.at[n]))
        copies[-1].start()
    for copy in copies:
        copy.wait()


def side_tiles(nx, ny, at_tail, got_ref, acc_in, lim_ref, base_ref, out_ref, acc_ref, done, sems, stops):
    size = base_ref.shape[1]
    table = [jnp.where(at_tail, r, l) for l, r in zip(*edge_weights(size))]
    offset = jnp.where(at_tail, 8, 0)
    acc_ref[...] = acc_in[...]

    def tile(x, even_plane, acc, limits):
        v = base_ref[pl.ds(pl.multiple_of(x * 16 + offset, 8), 8), :]
        for k in range(3):
            v = v + table[k] * got_ref[pl.ds(k * nx + x, 1), :]
        done[x] = v
        return excess(acc, v, even_plane, limits)

    def pair(j, _):
        limits = [jnp.broadcast_to(lim_ref[l : l + 1, :], (8, size)) for l in range(4)]
        acc = tile(2 * j, True, [acc_ref[l] for l in range(4)], limits)
        acc = tile(2 * j + 1, False, acc, limits)
        for l in range(4):
            acc_ref[l] = acc[l]
        return 0

    copies = []
    start = 0
    for i, stop in enumerate(stops):
        lax.fori_loop(start // 2, stop // 2, pair, 0, unroll=2)
        part = pl.ds(start, stop - start)
        rows = pl.ds(pl.multiple_of(jnp.where(at_tail, ny - 8, 0), 8), 8)
        copies.append(pltpu.make_async_copy(done.at[part], out_ref.at[part, rows, :], sems.at[i]))
        copies[-1].start()
        start = stop
    return copies


def inner_kernel(nx, ny, got_ref, acc_in, lim_ref, base_ref, out_in, out_ref, acc_ref, done, sems):
    del out_in
    at_tail = lax.axis_index("core") == 0
    stops = (nx // 2, nx)
    for copy in side_tiles(nx, ny, at_tail, got_ref, acc_in, lim_ref, base_ref, out_ref, acc_ref, done, sems, stops):
        copy.wait()


def outer_kernel(nx, ny, scale, got_ref, acc_in, lim_ref, base_ref, hot_ref, out_in, out_ref, mass_ref, acc_ref, done, sems):
    del out_in
    size = base_ref.shape[1]
    at_tail = lax.axis_index("core") != 0
    stops = (nx // 4, nx // 2, 3 * nx // 4, nx)
    copies = side_tiles(nx, ny, at_tail, got_ref, acc_in, lim_ref, base_ref, out_ref, acc_ref, done, sems, stops)
    blocks = 2
    width = size // blocks
    lines = []
    for c in range(blocks):
        for l in range(4):
            lines.append(jnp.sum(acc_ref[l, :, c * width : (c + 1) * width], axis=0, keepdims=True))
    sums = jnp.sum(jnp.concatenate(lines, axis=0), axis=1, keepdims=True)
    line = jnp.sum((sums * scale) * hot_ref[...], axis=0, keepdims=True)
    for i in range(mass_ref.shape[0]):
        mass_ref[i] = line
    for copy in copies:
        copy.wait()


def spread_kernel(parts_ref, out_ref):
    total = parts_ref[0]
    for i in range(1, parts_ref.shape[0]):
        total = total + parts_ref[i]
    for i in range(out_ref.shape[0]):
        out_ref[i] = total


def pair_swaps(n):
    inner = [(i, i ^ 1) for i in range(n)]
    return inner, [((i + 1) % n, (j + 1) % n) for i, j in inner]


def exchange(outer, inner, axes):
    swap_inner, swap_outer = pair_swaps(lax.axis_size(axes))
    outer = lax.ppermute(outer, axes, swap_outer)
    inner = lax.ppermute(inner, axes, swap_inner)
    return outer, inner


def near(*values):
    return [pltpu.with_memory_space_constraint(v, pltpu.VMEM) for v in values]


def far(value):
    return pltpu.with_memory_space_constraint(value, pltpu.HBM)


def cost(flops):
    return pl.CostEstimate(flops=flops, bytes_accessed=4 << 20, transcendentals=0)


def shards(pressure, cut_exponent, group_map):
    nx, ny, size = pressure.shape
    flat = pressure.reshape(nx * ny, size)
    blocks_z = cut_exponent.shape[2]
    table = jnp.asarray(lane_table(size))
    edge = pl.pallas_call(
        functools.partial(edge_kernel, nx, ny),
        out_shape=(in_vmem((3 * ny, size)), in_vmem((3 * ny, size))),
        in_specs=[ANY],
        out_specs=(VMEM, VMEM),
        scratch_shapes=[pltpu.VMEM((5 * ny, size), F32), pltpu.VMEM((6 * ny, size), F32), pltpu.SemaphoreType.DMA((2,))],
        compiler_params=PARAMS,
        name="edge",
    )
    outer, inner = edge(far(flat))
    later, outer, inner = lax.optimization_barrier((flat, outer, inner))
    got_outer, got_inner = exchange(outer, inner, ROW)
    bulk = pl.pallas_call(
        functools.partial(bulk_kernel, nx, ny),
        out_shape=(
            in_vmem((nx * ny, size)),
            in_vmem((3 * nx, size)),
            in_vmem((3 * nx, size)),
            in_vmem((size, size), jnp.bfloat16),
        ),
        in_specs=[VMEM, ANY],
        out_specs=(VMEM,) * 4,
        scratch_shapes=[pltpu.SemaphoreType.DMA],
        cost_estimate=cost(40_000_000),
        compiler_params=PARAMS,
        name="bulk",
    )
    work, inner, outer, table = bulk(*near(later), far(table))
    plane = pl.pallas_call(
        functools.partial(plane_kernel, nx, ny),
        out_shape=(in_vmem((3 * nx, size)), in_vmem((3 * nx, size))),
        in_specs=[VMEM] * 5,
        out_specs=(VMEM, VMEM),
        scratch_shapes=[pltpu.VMEM((40, size), F32)],
        compiler_params=PARAMS,
        name="plane",
    )
    inner, outer = plane(*near(got_outer, got_inner, table, inner, outer))
    outer, inner = exchange(outer, inner, COL)
    rows = pl.pallas_call(
        functools.partial(rows_kernel, nx, ny),
        out_shape=(
            jax.ShapeDtypeStruct((nx, ny, size), F32),
            in_vmem((nx * 16, size)),
            in_vmem((4, 8, size)),
            in_vmem((4, size)),
            in_vmem((8, 128)),
        ),
        in_specs=[VMEM] * 6,
        out_specs=(ANY, *(VMEM,) * 4),
        scratch_shapes=[
            pltpu.VMEM((6 * ny, size), F32),
            pltpu.VMEM((12 * ny, size), F32),
            pltpu.VMEM((nx, ny - 16, size), F32),
            pltpu.SemaphoreType.DMA((4,)),
        ],
        cost_estimate=cost(40_000_000),
        compiler_params=PARAMS,
        name="rows",
    )
    coeffs, base, acc, limits, hot = rows(
        *near(work, got_outer, got_inner, table, cut_exponent.reshape(1, blocks_z), group_map.reshape(1, blocks_z))
    )
    n_first, n_second = lax.axis_size(FIRST), lax.axis_size(SECOND)
    scale = 1.0 / (nx * ny * (size // blocks_z))
    inner_side = pl.pallas_call(
        functools.partial(inner_kernel, nx, ny),
        out_shape=(jax.ShapeDtypeStruct((nx, ny, size), F32), in_vmem((4, 8, size))),
        in_specs=[VMEM] * 4 + [ANY],
        out_specs=(ANY, VMEM),
        input_output_aliases={4: 0},
        scratch_shapes=[pltpu.VMEM((nx, 8, size), F32), pltpu.SemaphoreType.DMA((2,))],
        cost_estimate=cost(10_000_000),
        compiler_params=PARAMS,
        name="inner_side",
    )
    coeffs, acc = inner_side(*near(inner, acc, limits, base), coeffs)
    outer_side = pl.pallas_call(
        functools.partial(outer_kernel, nx, ny, scale),
        out_shape=(jax.ShapeDtypeStruct((nx, ny, size), F32), in_vmem((n_first, 1, 128))),
        in_specs=[VMEM] * 5 + [ANY],
        out_specs=(ANY, VMEM),
        input_output_aliases={5: 0},
        scratch_shapes=[
            pltpu.VMEM((4, 8, size), F32),
            pltpu.VMEM((nx, 8, size), F32),
            pltpu.SemaphoreType.DMA((4,)),
        ],
        compiler_params=PARAMS,
        name="outer_side",
    )
    coeffs, mass = outer_side(*near(outer, acc, limits, base, hot), coeffs)
    spread = pl.pallas_call(
        spread_kernel,
        out_shape=in_vmem((n_second, 1, 128)),
        in_specs=[VMEM],
        out_specs=VMEM,
        compiler_params=PARAMS,
        name="spread",
    )
    mass = spread(*near(lax.all_to_all(mass, FIRST, 0, 0)))
    mass = lax.all_to_all(mass, SECOND, 0, 0).sum(0)
    return coeffs, mass[0, : 4 * GROUPS].reshape(4, GROUPS).T


def solution(mesh):
    rows, cols = mesh.devices.shape
    z, y_hi = rows // 2, max(cols // 8, 1)
    devices = mesh.devices.reshape(z, 2, y_hi, cols // 2 // y_hi, 2)
    split = P(ROW, COL, None)
    return jax.shard_map(
        shards,
        mesh=Mesh(devices, ROW + COL),
        in_specs=(split, split, split),
        out_specs=(split, P()),
        check_vma=False,
    )
```

```python
import functools

import jax
import jax.numpy as jnp
import numpy as np
from jax import lax
from jax.experimental import pallas as pl
from jax.experimental.pallas import tpu as pltpu
from jax.sharding import Mesh
from jax.sharding import PartitionSpec as P

GROUPS = 16
ROW = ("z", "y_lo")
COL = ("y_hi", "x", "core")
FIRST = ("z", "core")
SECOND = ("y_hi", "y_lo", "x")
LEVELS = (0.25, 0.5, 1.0, 2.0)
A, B, C, G = 0.5625, 0.0625, 0.28125, 0.03125
F32 = jnp.float32
VMEM = pl.BlockSpec(memory_space=pltpu.VMEM)
PARAMS = pltpu.CompilerParams(vmem_limit_bytes=16 << 20)
ANY = pl.BlockSpec(memory_space=pl.ANY)


def in_vmem(shape, dtype=F32):
    return pltpu.VMEM(shape, dtype)


def lane_lift(v):
    size = v.shape[-1]
    odd = lax.broadcasted_iota(jnp.int32, v.shape, 1) % 2 == 1
    near = pltpu.roll(v, 1, axis=1) + pltpu.roll(v, size - 1, axis=1)
    far = pltpu.roll(v, 3, axis=1) + pltpu.roll(v, size - 3, axis=1)
    w = jnp.where(odd, v - (A * near - B * far), v)
    near = pltpu.roll(w, 1, axis=1) + pltpu.roll(w, size - 1, axis=1)
    far = pltpu.roll(w, 3, axis=1) + pltpu.roll(w, size - 3, axis=1)
    return jnp.where(odd, w, w + (C * near - G * far))


def lane_table(size):
    shift = lambda m, by: np.roll(m, by, axis=1)
    ident = np.eye(size)
    e, o = ident[:, 0::2], ident[:, 1::2]
    d = o - A * (e + shift(e, -1)) + B * (shift(e, 1) + shift(e, -2))
    s = e + C * (shift(d, 1) + d) - G * (shift(d, 2) + shift(d, -1))
    return np.stack([s, d], axis=2).reshape(size, size).astype(jnp.bfloat16)


def table_lift(v, table, pieces=2):
    total = None
    for _ in range(pieces):
        piece = v.astype(jnp.bfloat16)
        v = v - piece.astype(F32)
        term = jnp.dot(piece, table, preferred_element_type=F32)
        total = term if total is None else total + term
    return total


def to_right(at):
    e0, o0, e1, o1, e2 = at(2), at(1), at(4), at(3), at(6)
    return e0, o0 - A * e0 + B * e1, o1 - A * (e1 + e0) + B * e2


def to_left(at):
    e0, o0, e1, e2 = at(0), at(1), at(2), at(4)
    return e0, e1, o0 - A * (e0 + e1) + B * e2


FROM_LEFT = {0: (C * B, C, -G), 1: (B, 0.0, 0.0), 2: (C * B, -G, 0.0), 4: (-G * B, 0.0, 0.0)}
FROM_RIGHT = {
    6: (-G * B, 0.0, 0.0),
    4: (C * B + G * A, -G * B, 0.0),
    3: (B, 0.0, 0.0),
    2: (C * (B - A), C * B, -G),
    1: (-A, B, 0.0),
}


def combine(coefs, lines):
    total = None
    for coef, line in zip(coefs, lines):
        if coef != 0.0:
            term = coef * line
            total = term if total is None else total + term
    return total


def edge_kernel(nx, ny, p_ref, outer_ref, inner_ref, first, last, sems):
    lo = pltpu.make_async_copy(p_ref.at[pl.ds(0, 5 * ny)], first, sems.at[0])
    hi = pltpu.make_async_copy(p_ref.at[pl.ds((nx - 6) * ny, 6 * ny)], last, sems.at[1])
    lo.start()
    hi.start()
    even = lax.axis_index("y_lo") == 0
    lo.wait()
    hi.wait()
    left = to_left(lambda i: first[pl.ds(i * ny, ny), :])
    right = to_right(lambda i: last[pl.ds((6 - i) * ny, ny), :])
    for k, (r, l) in enumerate(zip(right, left)):
        outer_ref[pl.ds(k * ny, ny), :] = jnp.where(even, l, r)
        inner_ref[pl.ds(k * ny, ny), :] = jnp.where(even, r, l)


def boundary_lines(head, tail):
    return (*to_right(lambda i: tail[8 - i : 9 - i, :]), *to_left(lambda i: head[i : i + 1, :]))


def edge_weights(size):
    row = lax.broadcasted_iota(jnp.int32, (8, size), 0)

    def weights(table, place, k):
        total = jnp.zeros((8, size), F32)
        for line, coefs in table.items():
            if coefs[k] != 0.0:
                total = jnp.where(row == place(line), coefs[k], total)
        return total

    head = [weights(FROM_LEFT, lambda i: i, k) for k in range(3)]
    return head, [weights(FROM_RIGHT, lambda i: 8 - i, k) for k in range(3)]


def bulk_kernel(nx, ny, p_ref, table_hbm, w_ref, inner_ref, outer_ref, table_ref, sem):
    copy = pltpu.make_async_copy(table_hbm, table_ref, sem)
    copy.start()
    half = nx // 2
    tiles = w_ref.shape[1] // 128

    def column(i, _):
        lanes = pl.ds(pl.multiple_of(i % tiles * 128, 128), 128)
        rows = lambda x: pl.ds(pl.multiple_of(x * ny + i // tiles * 8, 8), 8)
        e = [p_ref[rows(2 * j), lanes] for j in range(half)]
        d = {-2: B * e[0], -1: B * e[1] - A * e[0], half: B * e[half - 1]}
        for j in range(half):
            near = e[j] + e[j + 1] if j + 1 < half else e[j]
            v = p_ref[rows(2 * j + 1), lanes] - A * near
            far = [e[i] for i in (j - 1, j + 2) if 0 <= i < half]
            if far:
                v = v + B * functools.reduce(lambda a, b: a + b, far)
            d[j] = v
            w_ref[rows(2 * j + 1), lanes] = v
        for j in range(half):
            w_ref[rows(2 * j), lanes] = e[j] + (C * (d[j - 1] + d[j]) - G * (d[j - 2] + d[j + 1]))
        return 0

    lax.fori_loop(0, ny // 8 * tiles, column, 0, unroll=2)
    copy.wait()
    size = nx * ny // 4
    for i in range(4):
        part = pl.ds(i * size, size)
        w_ref[part, :] = table_lift(w_ref[part, :], table_ref[...], 3)
    even = lax.axis_index("core") == 0

    def partial(x, _):
        head = w_ref[pl.ds(pl.multiple_of(x * ny, 8), 8), :]
        tail = w_ref[pl.ds(pl.multiple_of(x * ny + ny - 8, 8), 8), :]
        lines = boundary_lines(head, tail)
        for k, (right, left) in enumerate(zip(lines[:3], lines[3:])):
            inner_ref[pl.ds(k * nx + x, 1), :] = jnp.where(even, right, left)
            outer_ref[pl.ds(k * nx + x, 1), :] = jnp.where(even, left, right)
        return 0

    lax.fori_loop(0, nx, partial, 0, unroll=8)


def plane_kernel(nx, ny, got_o_ref, got_i_ref, table_ref, inner_in, outer_in, inner_ref, outer_ref, lines):
    size = table_ref.shape[0]
    even = lax.axis_index("core") == 0
    lines[...] = jnp.zeros_like(lines)
    y_even = lax.axis_index("y_lo") == 0
    for h in range(6):
        at = h % 3 * ny
        of_even, of_odd = (got_o_ref, got_i_ref) if h < 3 else (got_i_ref, got_o_ref)
        got = lambda part: jnp.where(y_even, of_even[part, :], of_odd[part, :])
        for m, line in enumerate(boundary_lines(got(slice(at, at + 8)), got(slice(at + ny - 8, at + ny)))):
            lines[6 * h + m : 6 * h + m + 1, :] = line
    lines[...] = table_lift(lines[...], table_ref[...])
    inner_ref[...] = inner_in[...]
    outer_ref[...] = outer_in[...]
    for first, at, weights in zip((0, 3), (0, nx - 8), edge_weights(size)):
        for k in range(3):
            row = lambda h, m: lines[6 * h + m : 6 * h + m + 1, :]
            right = sum(weights[i] * row(first + i, k) for i in range(3))
            left = sum(weights[i] * row(first + i, 3 + k) for i in range(3))
            part = slice(k * nx + at, k * nx + at + 8)
            inner_ref[part, :] = inner_ref[part, :] + jnp.where(even, right, left)
            outer_ref[part, :] = outer_ref[part, :] + jnp.where(even, left, right)


def excess(acc, v, even_plane, limits):
    m = jnp.abs(v)
    if even_plane:
        row = lax.broadcasted_iota(jnp.int32, v.shape, 0)
        lane = lax.broadcasted_iota(jnp.int32, v.shape, 1)
        m = jnp.where((row | lane) % 2 == 1, m, 0.0)
    return [a + jnp.maximum(m - lim, 0.0) for a, lim in zip(acc, limits)]


def rows_kernel(nx, ny, w_ref, got_o_ref, got_i_ref, table_ref, cut_ref, group_ref, out_ref, edge_ref, acc_ref, lim_ref, hot_ref, halo, fixed_ref, mid, sems):
    size = w_ref.shape[1]
    blocks = cut_ref.shape[1]
    lane = lax.broadcasted_iota(jnp.int32, (1, size), 1)
    cut = jnp.zeros((1, size), jnp.int32)
    place = lax.broadcasted_iota(jnp.int32, (8, 128), 0)
    group = jnp.zeros((8, 128), jnp.int32)
    for c in range(blocks):
        cut = jnp.where(lane // (size // blocks) == c, cut_ref[:, c : c + 1], cut)
        group = jnp.where(place // 4 == c, group_ref[:, c : c + 1], group)
    scales = jnp.exp2(-cut.astype(F32))
    for l, level in enumerate(LEVELS):
        lim_ref[l : l + 1, :] = level * scales
    hot = lax.broadcasted_iota(jnp.int32, (8, 128), 1) == GROUPS * (place % 4) + group
    hot_ref[...] = jnp.where(hot, 1.0, 0.0)
    acc_ref[...] = jnp.zeros_like(acc_ref)

    y_even = lax.axis_index("y_lo") == 0
    halo[pl.ds(0, 3 * ny), :] = table_lift(jnp.where(y_even, got_o_ref[...], got_i_ref[...]), table_ref[...])
    halo[pl.ds(3 * ny, 3 * ny), :] = table_lift(jnp.where(y_even, got_i_ref[...], got_o_ref[...]), table_ref[...])

    def fix(t, _):
        rows = lambda x: pl.ds(pl.multiple_of(x * ny + t * 8, 8), 8)
        lines = [halo[rows(k), :] for k in range(3)]
        for x in range(6):
            v = w_ref[rows(x), :]
            fixed_ref[rows(x), :] = v + combine(FROM_LEFT[x], lines) if x in FROM_LEFT else v
        lines = [halo[rows(3 + k), :] for k in range(3)]
        for back in range(6, 0, -1):
            v = w_ref[rows(nx - back), :]
            fixed_ref[rows(12 - back), :] = v + combine(FROM_RIGHT[back], lines) if back in FROM_RIGHT else v
        return 0

    lax.fori_loop(0, ny // 8, fix, 0)

    def lift(src, at_plane):
        v = src[pl.ds(pl.multiple_of(at_plane * ny, 8), ny), :]
        v = jnp.concatenate([v, jnp.zeros((8, size), F32)], axis=0)
        odd = lax.broadcasted_iota(jnp.int32, v.shape, 0) % 2 == 1
        at = lambda u, by: pltpu.roll(u, by % (ny + 8), axis=0)
        w = jnp.where(odd, v - (A * (at(v, 1) + at(v, -1)) - B * (at(v, 3) + at(v, -3))), v)
        s = w + (C * (at(w, 1) + at(w, -1)) - G * (at(w, 3) + at(w, -3)))
        return jnp.where(odd, w, s)[0:ny, :]

    def plane(src, at_plane, x, even_plane):
        v = lift(src, at_plane)
        edge_ref[pl.ds(pl.multiple_of(x * 16, 8), 8), :] = v[0:8, :]
        edge_ref[pl.ds(pl.multiple_of(x * 16 + 8, 8), 8), :] = v[ny - 8 : ny, :]
        mid[x] = v[8 : ny - 8, :]
        limits = [jnp.broadcast_to(lim_ref[l : l + 1, :], (8, size)) for l in range(4)]
        acc = [acc_ref[l] for l in range(4)]
        for t in range(1, ny // 8 - 1):
            acc = excess(acc, v[8 * t : 8 * t + 8, :], even_plane, limits)
        for l in range(4):
            acc_ref[l] = acc[l]

    copies = []
    middle = (nx - 12) // 2
    for n, (src, start, x0, each) in enumerate(
        ((fixed_ref, 0, 0, 6), (w_ref, 6, 6, middle), (w_ref, 6 + middle, 6 + middle, middle), (fixed_ref, 6, nx - 6, 6))
    ):

        def pair(j, _):
            plane(src, start + 2 * j, x0 + 2 * j, True)
            plane(src, start + 2 * j + 1, x0 + 2 * j + 1, False)
            return 0

        lax.fori_loop(0, each // 2, pair, 0)
        part = pl.ds(x0, each)
        copies.append(pltpu.make_async_copy(mid.at[part], out_ref.at[part, pl.ds(8, ny - 16), :], sems.at[n]))
        copies[-1].start()
    for copy in copies:
        copy.wait()


def final_kernel(nx, ny, scale, outer_ref, inner_ref, acc_in, lim_ref, hot_ref, base_ref, out_in, out_ref, mass_ref, acc_ref, done, sems):
    del out_in
    size = base_ref.shape[1]
    from_l, from_r = edge_weights(size)
    acc_ref[...] = acc_in[...]
    even = lax.axis_index("core") == 0

    def tiles(x, even_plane):
        limits = [jnp.broadcast_to(lim_ref[l : l + 1, :], (8, size)) for l in range(4)]
        acc = [acc_ref[l] for l in range(4)]
        inner = [inner_ref[pl.ds(k * nx + x, 1), :] for k in range(3)]
        outer = [outer_ref[pl.ds(k * nx + x, 1), :] for k in range(3)]
        left = [jnp.where(even, o, i) for i, o in zip(inner, outer)]
        right = [jnp.where(even, i, o) for i, o in zip(inner, outer)]
        for n, got, table in ((0, left, from_l), (1, right, from_r)):
            v = base_ref[pl.ds(pl.multiple_of(x * 16 + 8 * n, 8), 8), :]
            for k in range(3):
                v = v + table[k] * got[k]
            done[n, x] = v
            acc = excess(acc, v, even_plane, limits)
        for l in range(4):
            acc_ref[l] = acc[l]

    def pair(j, _):
        tiles(2 * j, True)
        tiles(2 * j + 1, False)
        return 0

    copies = []
    start = 0
    for i, stop in enumerate((4, 12, 20, nx - 4, nx)):
        lax.fori_loop(start // 2, stop // 2, pair, 0, unroll=2)
        part = pl.ds(start, stop - start)
        for n, at in enumerate((0, ny - 8)):
            copies.append(pltpu.make_async_copy(done.at[n, part], out_ref.at[part, pl.ds(at, 8), :], sems.at[2 * i + n]))
            copies[-1].start()
        start = stop
    blocks = 2
    width = size // blocks
    lines = []
    for c in range(blocks):
        for l in range(4):
            lines.append(jnp.sum(acc_ref[l, :, c * width : (c + 1) * width], axis=0, keepdims=True))
    sums = jnp.sum(jnp.concatenate(lines, axis=0), axis=1, keepdims=True)
    line = jnp.sum((sums * scale) * hot_ref[...], axis=0, keepdims=True)
    for i in range(mass_ref.shape[0]):
        mass_ref[i] = line
    for copy in copies:
        copy.wait()


def spread_kernel(parts_ref, out_ref):
    total = parts_ref[0]
    for i in range(1, parts_ref.shape[0]):
        total = total + parts_ref[i]
    for i in range(out_ref.shape[0]):
        out_ref[i] = total


def pair_swaps(n):
    inner = [(i, i ^ 1) for i in range(n)]
    return inner, [((i + 1) % n, (j + 1) % n) for i, j in inner]


def exchange(outer, inner, axes):
    swap_inner, swap_outer = pair_swaps(lax.axis_size(axes))
    inner = lax.ppermute(inner, axes, swap_inner)
    return lax.ppermute(outer, axes, swap_outer), inner


def near(*values):
    return [pltpu.with_memory_space_constraint(v, pltpu.VMEM) for v in values]


def far(value):
    return pltpu.with_memory_space_constraint(value, pltpu.HBM)


def cost(flops):
    return pl.CostEstimate(flops=flops, bytes_accessed=4 << 20, transcendentals=0)


def shards(pressure, cut_exponent, group_map):
    nx, ny, size = pressure.shape
    flat = pressure.reshape(nx * ny, size)
    blocks_z = cut_exponent.shape[2]
    table = jnp.asarray(lane_table(size))
    edge = pl.pallas_call(
        functools.partial(edge_kernel, nx, ny),
        out_shape=(in_vmem((3 * ny, size)), in_vmem((3 * ny, size))),
        in_specs=[ANY],
        out_specs=(VMEM, VMEM),
        scratch_shapes=[pltpu.VMEM((5 * ny, size), F32), pltpu.VMEM((6 * ny, size), F32), pltpu.SemaphoreType.DMA((2,))],
        compiler_params=PARAMS,
        name="edge",
    )
    outer, inner = edge(far(flat))
    later, outer, inner = lax.optimization_barrier((flat, outer, inner))
    got_outer, got_inner = exchange(outer, inner, ROW)
    bulk = pl.pallas_call(
        functools.partial(bulk_kernel, nx, ny),
        out_shape=(
            in_vmem((nx * ny, size)),
            in_vmem((3 * nx, size)),
            in_vmem((3 * nx, size)),
            in_vmem((size, size), jnp.bfloat16),
        ),
        in_specs=[VMEM, ANY],
        out_specs=(VMEM,) * 4,
        scratch_shapes=[pltpu.SemaphoreType.DMA],
        cost_estimate=cost(40_000_000),
        compiler_params=PARAMS,
        name="bulk",
    )
    work, inner, outer, table = bulk(*near(later), far(table))
    plane = pl.pallas_call(
        functools.partial(plane_kernel, nx, ny),
        out_shape=(in_vmem((3 * nx, size)), in_vmem((3 * nx, size))),
        in_specs=[VMEM] * 5,
        out_specs=(VMEM, VMEM),
        scratch_shapes=[pltpu.VMEM((40, size), F32)],
        compiler_params=PARAMS,
        name="plane",
    )
    inner, outer = plane(*near(got_outer, got_inner, table, inner, outer))
    outer, inner = exchange(outer, inner, COL)
    rows = pl.pallas_call(
        functools.partial(rows_kernel, nx, ny),
        out_shape=(
            jax.ShapeDtypeStruct((nx, ny, size), F32),
            in_vmem((nx * 16, size)),
            in_vmem((4, 8, size)),
            in_vmem((4, size)),
            in_vmem((8, 128)),
        ),
        in_specs=[VMEM] * 6,
        out_specs=(ANY, *(VMEM,) * 4),
        scratch_shapes=[
            pltpu.VMEM((6 * ny, size), F32),
            pltpu.VMEM((12 * ny, size), F32),
            pltpu.VMEM((nx, ny - 16, size), F32),
            pltpu.SemaphoreType.DMA((4,)),
        ],
        cost_estimate=cost(40_000_000),
        compiler_params=PARAMS,
        name="rows",
    )
    coeffs, base, acc, limits, hot = rows(
        *near(work, got_outer, got_inner, table, cut_exponent.reshape(1, blocks_z), group_map.reshape(1, blocks_z))
    )
    n_first, n_second = lax.axis_size(FIRST), lax.axis_size(SECOND)
    scale = 1.0 / (nx * ny * (size // blocks_z))
    final = pl.pallas_call(
        functools.partial(final_kernel, nx, ny, scale),
        out_shape=(jax.ShapeDtypeStruct((nx, ny, size), F32), in_vmem((n_first, 1, 128))),
        in_specs=[VMEM] * 6 + [ANY],
        out_specs=(ANY, VMEM),
        input_output_aliases={6: 0},
        scratch_shapes=[
            pltpu.VMEM((4, 8, size), F32),
            pltpu.VMEM((2, nx, 8, size), F32),
            pltpu.SemaphoreType.DMA((10,)),
        ],
        compiler_params=PARAMS,
        name="final",
    )
    coeffs, mass = final(*near(outer, inner, acc, limits, hot, base), coeffs)
    spread = pl.pallas_call(
        spread_kernel,
        out_shape=in_vmem((n_second, 1, 128)),
        in_specs=[VMEM],
        out_specs=VMEM,
        compiler_params=PARAMS,
        name="spread",
    )
    mass = spread(*near(lax.all_to_all(mass, FIRST, 0, 0)))
    mass = lax.all_to_all(mass, SECOND, 0, 0).sum(0)
    return coeffs, mass[0, : 4 * GROUPS].reshape(4, GROUPS).T


def solution(mesh):
    rows, cols = mesh.devices.shape
    z, y_hi = rows // 2, max(cols // 8, 1)
    devices = mesh.devices.reshape(z, 2, y_hi, cols // 2 // y_hi, 2)
    split = P(ROW, COL, None)
    return jax.shard_map(
        shards,
        mesh=Mesh(devices, ROW + COL),
        in_specs=(split, split, split),
        out_specs=(split, P()),
        check_vma=False,
    )
```
